256 devices in a mesh: dp: 4 (over x), expert: 32 (over y, z), tensor: 2 (over core).
Axes of the slice: x: 4, y: 4, z: 8, core: 2. Of those that a mesh axis runs over, the one named last changes fastest.
Arguments:
- tokens: bfloat16 [16384, 2560], P(('dp', 'expert')), may hold values from -6 to 6
- norm_gain: float32 [2560], replicated, may hold values from 0.5 to 1.5
- expert_ids: int32 [16384, 6], P(('dp', 'expert')), may hold values from 0 to 31, all different within a row; in each aligned block of 128 rows (0 to 127, 128 to 255, ...) at most 48 rows name the same one
- route_weights: int32 [16384, 6], P(('dp', 'expert')), may hold values from 1 to 64
- w_gate: bfloat16 [32, 2560, 768], P('expert', None, 'tensor'), may hold values from -0.125 to 0.125
- w_up: bfloat16 [32, 2560, 768], P('expert', None, 'tensor'), may hold values from -0.125 to 0.125
- w_down: bfloat16 [32, 768, 2560], P('expert', 'tensor'), may hold values from -0.21875 to 0.21875
- shared_gate: bfloat16 [2560, 2048], P(None, ('dp', 'tensor')), may hold values from -0.125 to 0.125
- shared_up: bfloat16 [2560, 2048], P(None, ('dp', 'tensor')), may hold values from -0.125 to 0.125
- shared_down: bfloat16 [2048, 2560], P(('dp', 'tensor')), may hold values from -0.125 to 0.125
Outputs:
- mixed: bfloat16 [16384, 2560], P(('dp', 'expert'), 'tensor')
The draws below stay inside these ranges and needn't reach their ends.
Inputs may be any that keep to these rules, and one draw needn't show every extreme that they name: `expert_ids`: each row names 6 different experts. In each aligned block of 128 rows (the rows of one index of dp+expert) no expert is named by more than 48 rows, a bound that some blocks reach.
All inputs are finite; a program needn't handle non-finite values.
Results may differ from the reference program's by a relative error of at most 0.011.
Values may be sent and summed in bfloat16 or wider, within the bound.
A program may use at most 128 MiB of HBM per device.

```python
import math
import jax
import jax.numpy as jnp
import numpy as np
from jax import lax

D = 2560
FF = 768
SFF = 2048
EXPERTS = 32
TOP = 6
TOK_DEV = 128
CAP = 48
TOKENS = 16384


def place_ends(values, own_key, low, largest):
    spot = [jax.random.randint(jax.random.fold_in(own_key, axis), (), 0, length) for axis, length in enumerate(values.shape)]
    widest = values.shape.index(max(values.shape))
    next_to = spot[:widest] + [(spot[widest] + 1) % values.shape[widest]] + spot[widest + 1:]
    return values.at[tuple(spot)].set(low).at[tuple(next_to)].set(largest)


def shard_levels(rng, extent, split, low, largest):
    loudness = 1.0
    for dim, parts in split:
        draws = jax.random.uniform(jax.random.fold_in(jax.random.fold_in(rng, 6), dim), (parts,), jnp.float32, low / len(split), largest / len(split))
        loudness = loudness * jnp.repeat(jnp.exp(draws), extent[dim] // parts).reshape((-1,) + (1,) * (len(extent) - 1 - dim))
    return loudness


def deal_out(key, own, number, rows, number_of, top, reach, slope):
    ranking = jax.random.permutation(key, number_of)
    crowded, usual = portions_of(number_of, rows * top, reach, slope, True), portions_of(number_of, rows * top, reach, slope, False)
    places = jnp.arange(number_of)

    def named(tallies, offset_by):
        used = int((tallies > 0).sum())
        fixed = max(1, used // 4)
        shifted = fixed + (places - fixed + offset_by * (used - fixed)) % max(1, number_of - fixed)
        return jnp.zeros((number_of,), jnp.int32).at[ranking[jnp.where(places < fixed, places, shifted)]].set(jnp.asarray(tallies, jnp.int32))

    tallies = jnp.where(number % 4 == 0, named(crowded, number // 4), named(usual, number - number // 4 - 1))
    mixed = jax.random.permutation(jax.random.fold_in(own, 3), number_of)
    donor, taker = mixed[0:number_of // 2 * 2:2], mixed[1:number_of // 2 * 2:2]
    slack = jnp.minimum(tallies[donor] - 1, reach - tallies[taker]) // 2
    slack = jnp.where((donor == ranking[0]) | (taker == ranking[0]) | (tallies[taker] == 0), 0, jnp.maximum(slack, 0))
    shifted = jax.random.randint(jax.random.fold_in(own, 4), (number_of // 2,), 0, 1 << 20) % (slack + 1)
    tallies = tallies.at[donor].add(-shifted).at[taker].add(shifted)
    labels = jnp.searchsorted(jnp.cumsum(tallies), jnp.arange(rows * top), side="right").astype(jnp.int32)
    table = labels.reshape(top, rows).T
    table = table[jax.random.permutation(jax.random.fold_in(own, 1), rows)]
    offset_by = jax.random.randint(jax.random.fold_in(own, 2), (rows, 1), 0, top)
    return jnp.take_along_axis(table, (jnp.arange(top)[None, :] + offset_by) % top, axis=1)


def portions_of(count, total, limit, skew, full):
    portions = [(1 << 20) // math.isqrt(standing ** skew) + 1 for standing in range(1, count + 1)]
    largest = limit if full else min(limit, max(-(-total // count), total * portions[0] // sum(portions)))
    least = 1 if total - largest >= count - 1 else 0
    holding, rest = [largest] + [least] * (count - 1), total - largest - least * (count - 1)
    while rest > 0:
        movable = [i for i in range(1, count) if holding[i] < largest] or [i for i in range(1, count) if holding[i] < limit]
        pool, left = sum([portions[i] for i in movable]), rest
        for i in movable:
            extra = min(limit - holding[i], max(1, left * portions[i] // pool), rest)
            holding[i] = holding[i] + extra
            rest = rest - extra
    return np.array(holding)


def bell_draw(rng, dims, deviation, bound, cuts=(), kind=jnp.bfloat16):
    values = jax.random.normal(rng, dims, jnp.float32) * deviation
    if len(cuts) > 0:
        values = shard_levels(rng, dims, cuts, -0.22, 0.18) * values
    return jnp.clip(values, min=-bound, max=bound).astype(kind)


def setup_inputs(seed: int = 0) -> dict:
    keys = jax.random.split(jax.random.key(seed), 11)
    tokens = bell_draw(keys[0], (TOKENS, D), 1.0, 6.0, ((0, 128),))
    norm_gain = jnp.clip(1.0 + 0.1 * jax.random.normal(keys[1], (D,), jnp.float32), 0.5, 1.5)
    expert_ids_keys = jax.random.split(jax.random.fold_in(keys[2], 1), TOKENS // TOK_DEV)
    expert_ids_turns = jax.random.permutation(jax.random.fold_in(keys[2], 3), TOKENS // TOK_DEV)
    expert_ids = jax.vmap(lambda own, number: deal_out(jax.random.fold_in(keys[2], 2), own, number, TOK_DEV, EXPERTS, TOP, CAP, 2))(expert_ids_keys, expert_ids_turns).reshape((TOKENS, TOP))
    route_weights = place_ends(jax.random.randint(keys[3], (TOKENS, TOP), 1, 65), jax.random.fold_in(keys[3], 1), 1, 64).astype(jnp.int32)
    w_gate = bell_draw(keys[4], (EXPERTS, D, FF), D ** -0.5, 0.125, ((0, 32), (2, 2)))
    w_up = bell_draw(keys[5], (EXPERTS, D, FF), D ** -0.5, 0.125, ((0, 32), (2, 2)))
    w_down = bell_draw(keys[6], (EXPERTS, FF, D), FF ** -0.5, 0.21875, ((0, 32), (1, 2)))
    shared_gate = bell_draw(keys[7], (D, SFF), D ** -0.5, 0.125, ((1, 8),))
    shared_up = bell_draw(keys[8], (D, SFF), D ** -0.5, 0.125, ((1, 8),))
    shared_down = bell_draw(keys[9], (SFF, D), SFF ** -0.5, 0.125, ((0, 8),))
    return {"tokens": tokens, "norm_gain": norm_gain, "expert_ids": expert_ids, "route_weights": route_weights, "w_gate": w_gate, "w_up": w_up, "w_down": w_down, "shared_gate": shared_gate, "shared_up": shared_up, "shared_down": shared_down}


EPSILON = 1e-06

def normalize(tokens, norm_gain):
    values = tokens.astype(jnp.float32)
    inverse = lax.rsqrt(lax.optimization_barrier(jnp.mean(values * values, axis=1, keepdims=True)) + EPSILON)
    return (values * inverse * norm_gain.astype(jnp.float32)[None, :]).astype(jnp.bfloat16)

def reference(tokens, norm_gain, expert_ids, route_weights, w_gate, w_up, w_down, shared_gate, shared_up, shared_down):
    normed = normalize(tokens, norm_gain)
    groups = TOKENS // TOK_DEV
    pair_total = TOK_DEV * TOP
    local_ids = expert_ids.reshape(groups, pair_total).astype(jnp.int32)
    onehot = (local_ids[:, :, None] == jnp.arange(EXPERTS, dtype=jnp.int32)[None, None, :]).astype(jnp.int32)
    earlier = jnp.cumsum(onehot, axis=1) - onehot
    slot_index = lax.optimization_barrier(jnp.sum(earlier * onehot, axis=2)).astype(jnp.int32)
    position = (local_ids * CAP + slot_index).astype(jnp.int32)
    group_index = jnp.broadcast_to(jnp.arange(groups, dtype=jnp.int32)[:, None], (groups, pair_total)).astype(jnp.int32)
    pair_token = (group_index * TOK_DEV + jnp.arange(pair_total, dtype=jnp.int32)[None, :] // TOP).astype(jnp.int32)
    filler = jnp.full((groups, EXPERTS * CAP), -1, jnp.int32).at[group_index, position].set(pair_token)
    pair_scale = route_weights.astype(jnp.float32).reshape(groups, pair_total) / 64.0
    slot_scale = jnp.zeros((groups, EXPERTS * CAP), jnp.float32).at[group_index, position].set(pair_scale)
    filler = filler.reshape(groups, EXPERTS, CAP).transpose(1, 0, 2).reshape(EXPERTS, groups * CAP)
    slot_scale = slot_scale.reshape(groups, EXPERTS, CAP).transpose(1, 0, 2).reshape(EXPERTS, groups * CAP)

    def expert_step(totals, inputs):
        owner_rows, owner_scale, gate_weight, up_weight, down_weight = inputs
        valid = owner_rows >= 0
        safe_rows = jnp.maximum(owner_rows, 0).astype(jnp.int32)
        picked = jnp.where(valid[:, None], normed[safe_rows], jnp.zeros((), jnp.bfloat16))
        gate_value = jnp.dot(picked, gate_weight, preferred_element_type=jnp.float32)
        up_value = jnp.dot(picked, up_weight, preferred_element_type=jnp.float32)
        hidden = (jax.nn.silu(gate_value) * up_value).astype(jnp.bfloat16)
        result = jnp.dot(hidden, down_weight, preferred_element_type=jnp.float32).astype(jnp.bfloat16)
        update = result.astype(jnp.float32) * owner_scale[:, None]
        update = jnp.where(valid[:, None], update, jnp.zeros((), jnp.float32))
        return (totals.at[safe_rows].add(update), None)
    routed, unused = lax.scan(expert_step, jnp.zeros((TOKENS, D), jnp.float32), (filler, slot_scale, w_gate, w_up, w_down))
    shared_gate_value = jnp.dot(normed, shared_gate, preferred_element_type=jnp.float32)
    shared_up_value = jnp.dot(normed, shared_up, preferred_element_type=jnp.float32)
    shared_hidden = (jax.nn.silu(shared_gate_value) * shared_up_value).astype(jnp.bfloat16)
    shared_out = jnp.dot(shared_hidden, shared_down, preferred_element_type=jnp.float32)
    return (shared_out + routed).astype(jnp.bfloat16)
```

```python
import jax
import jax.numpy as jnp
from jax import lax
from jax.experimental import pallas as pl
from jax.experimental.pallas import tpu as pltpu
from jax.sharding import PartitionSpec as P

D = 2560
HALF = D // 2
QUARTER = HALF // 2
FF2 = 384
FF = 768
SF = 256
EXPERTS = 32
TOP = 6
TOK = 128
CAP = 48
YN = 4
ZN = 8
XN = 4
ROWS = YN * CAP
EPSILON = 1e-06
MESH = pl.DeviceIdType.MESH
BF16 = jnp.bfloat16
F32 = jnp.float32


def owner(d):
    return 0 if d < ZN // 2 else 1


def chunk_of(d):
    return d if d < ZN // 2 else ZN - 1 - d


def kernel(
    tokens, gain, ids, weights, wg_in, wu_in, wd_in, sg_in, su_in, sd_in,
    out,
    t_buf, g_buf, code, d_buf, r_buf, h_buf, o_buf, q_buf,
    plus_in, minus_in, plus_out, minus_out, sh_buf, s_in,
    wg, wu, wd, sgu, sd,
    load_sem, wsend_sem, wrecv_sem,
    zsend_sem, zrecv_sem, csend_sem, crecv_sem,
    ysend_sem, yrecv_sem, ysend0_sem, yrecv0_sem,
    bsend_sem, brecv_sem, bsend0_sem, brecv0_sem,
    rsend_sem, rrecv_sem,
    xsend_sem, xrecv_sem, ssend_sem, srecv_sem,
):
    x = lax.axis_index("dp")
    e = lax.axis_index("expert")
    r = lax.axis_index("tensor")
    y = e // ZN
    z = e % ZN
    half = pl.multiple_of(r * HALF, 128)
    other = pl.multiple_of((1 - r) * HALF, 128)

    def at(dx=0, dy=0, dz=0, core=None):
        return (
            (x + dx + XN) % XN,
            ((y + dy + YN) % YN) * ZN + (z + dz + ZN) % ZN,
            r if core is None else core,
        )

    partner = at(core=1 - r)

    def remote(src, dst, send, recv, device):
        return pltpu.make_async_remote_copy(
            src_ref=src, dst_ref=dst, send_sem=send, recv_sem=recv,
            device_id=device, device_id_type=MESH,
        )

    def await_bytes(ref, sem):
        pltpu.make_async_copy(ref, ref, sem).wait()

    barrier = pltpu.get_barrier_semaphore()
    peers = [partner, at(dz=1), at(dz=-1)]
    for k in range(1, YN):
        peers += [at(dy=k), at(dy=k, core=1 - r)]
    for k in range(1, XN):
        peers += [at(dx=k), at(dx=k, core=1 - r)]
    for peer in peers:
        pl.semaphore_signal(barrier, inc=1, device_id=peer, device_id_type=MESH)

    loads = [
        (wg_in.at[0], wg.at[:, pl.ds(0, FF2)]),
        (wu_in.at[0], wu.at[:, pl.ds(0, FF2)]),
        (wd_in.at[0], wd.at[pl.ds(0, FF2), :]),
        (sg_in, sgu.at[:, pl.ds(0, SF)]),
        (su_in, sgu.at[:, pl.ds(SF, SF)]),
        (sd_in, sd),
    ]
    for i, (src, dst) in enumerate(loads):
        pltpu.make_async_copy(src, dst, load_sem.at[i]).start()

    def norm_step(i, carry):
        rows = pl.ds(pl.multiple_of(i * 16, 16), 16)
        values = tokens[rows, :].astype(F32)
        inverse = lax.rsqrt(jnp.mean(values * values, axis=1, keepdims=True) + EPSILON)
        normed = values * inverse * gain[...]
        t_buf[0, rows, :] = normed.astype(BF16)
        g_buf[0, rows, :] = jnp.where(r == 0, normed[:, :HALF], normed[:, HALF:]).astype(BF16)
        return carry

    lax.fori_loop(0, TOK // 16, norm_step, 0)

    lane = lax.broadcasted_iota(jnp.int32, (TOK, 128), 1)
    row = lax.broadcasted_iota(jnp.int32, (TOK, 128), 0)
    named = jnp.zeros((TOK, 128), F32)
    weight = jnp.zeros((TOK, 128), F32)
    for k in range(TOP):
        match = ids[:, k : k + 1] == lane
        named = jnp.where(match, 1.0, named)
        weight = jnp.where(match, weights[:, k : k + 1].astype(F32), weight)
    earlier = jnp.where(lane < row, 1.0, 0.0).astype(BF16)
    rank = jnp.dot(earlier, named.astype(BF16), preferred_element_type=F32)
    packed = jnp.where(named > 0.5, weight * 64.0 + rank, -1.0)
    code[0] = packed.T[:EXPERTS, :]

    pl.semaphore_wait(barrier, len(peers))

    def z_copies(way, k):
        if way == 0:
            here, there, to = k - 1, k, at(dz=-1)
        else:
            here, there, to = (ZN - (k - 1)) % ZN, ZN - k, at(dz=1)
        if k == ZN // 2:
            cols = pl.ds(way * QUARTER, QUARTER)
            src, dst = g_buf.at[here, :, cols], g_buf.at[there, :, cols]
        else:
            src, dst = g_buf.at[here], g_buf.at[there]
        copies = [remote(src, dst, zsend_sem.at[way, k - 1], zrecv_sem.at[way, k - 1], to)]
        if k < ZN // 2 or way == 0:
            copies.append(
                remote(code.at[here], code.at[there], csend_sem.at[way, k - 1], crecv_sem.at[way, k - 1], to)
            )
        return copies

    def weight_copies():
        return [
            remote(wg_in.at[0], wg.at[:, pl.ds(FF2, FF2)], wsend_sem.at[0], wrecv_sem.at[0], partner),
            remote(wu_in.at[0], wu.at[:, pl.ds(FF2, FF2)], wsend_sem.at[1], wrecv_sem.at[1], partner),
            remote(wd_in.at[0], wd.at[pl.ds(FF2, FF2), :], wsend_sem.at[2], wrecv_sem.at[2], partner),
        ]

    def x_copy(k):
        return remote(t_buf.at[0], t_buf.at[k], xsend_sem.at[k - 1], xrecv_sem.at[k - 1], at(dx=k))

    for way in range(2):
        for copy in z_copies(way, 1):
            copy.start()

    slot = lax.broadcasted_iota(jnp.int32, (CAP, TOK), 0).astype(F32)

    def slot_parts(d):
        for k in range(YN):
            expert = ((y + k) % YN) * ZN + z
            line = code[d, pl.ds(expert, 1), :]
            scale = jnp.floor(line * (1.0 / 64.0))
            yield slot == line - 64.0 * scale, scale * (1.0 / 64.0)

    def y_copies(d):
        j, core = chunk_of(d), owner(d)
        return [
            remote(
                d_buf.at[d, pl.ds(CAP * k, CAP), :],
                r_buf.at[j, pl.ds(CAP * k, CAP), pl.ds(half, HALF)],
                ysend_sem.at[d], yrecv_sem.at[j], at(dy=k, core=core),
            )
            for k in range(1, YN)
        ]

    def y_own_copy(d):
        return remote(
            d_buf.at[d, pl.ds(0, CAP), :],
            r_buf.at[chunk_of(d), pl.ds(0, CAP), pl.ds(half, HALF)],
            ysend0_sem.at[d], yrecv0_sem.at[chunk_of(d)], partner,
        )

    def dispatch(d):
        pick = jnp.concatenate([jnp.where(hit, 1.0, 0.0) for hit, _ in slot_parts(d)], axis=0).astype(BF16)
        for cols in (pl.ds(0, QUARTER), pl.ds(QUARTER, QUARTER)):
            d_buf[d, :, cols] = jnp.dot(pick, g_buf[d, :, cols], preferred_element_type=F32).astype(BF16)
        for copy in y_copies(d):
            copy.start()

        @pl.when(r == owner(d))
        def _():
            r_buf[chunk_of(d), pl.ds(0, CAP), pl.ds(half, HALF)] = d_buf[d, pl.ds(0, CAP), :]

        @pl.when(r != owner(d))
        def _():
            y_own_copy(d).start()

    def z_arrived(k):
        for way in range(2):
            for copy in z_copies(way, k):
                copy.wait_recv()
            if k < ZN // 2:
                for copy in z_copies(way, k + 1):
                    copy.start()

    def experts(j):
        await_bytes(r_buf.at[j, pl.ds(CAP, 3 * CAP), :], yrecv_sem.at[j])
        await_bytes(r_buf.at[j, pl.ds(0, CAP), pl.ds(other, HALF)], yrecv0_sem.at[j])

        def up_step(n, carry):
            cols = pl.ds(pl.multiple_of(n * 256, 256), 256)
            gate_value = jnp.dot(r_buf[j], wg[:, cols], preferred_element_type=F32)
            up_value = jnp.dot(r_buf[j], wu[:, cols], preferred_element_type=F32)
            h_buf[:, cols] = (jax.nn.silu(gate_value) * up_value).astype(BF16)
            return carry

        lax.fori_loop(0, FF // 256, up_step, 0)

        def down_step(n, carry):
            cols = pl.ds(pl.multiple_of(n * 256, 256), 256)
            o_buf[j, :, cols] = jnp.dot(h_buf[...], wd[:, cols], preferred_element_type=F32).astype(BF16)
            return carry

        lax.fori_loop(0, D // 256, down_step, 0)

    def back_copies(j):
        d = jnp.where(r == 0, j, ZN - 1 - j)
        copies = []
        for k in range(1, YN):
            for cols, core in ((half, r), (other, 1 - r)):
                copies.append(
                    remote(
                        o_buf.at[j, pl.ds(CAP * k, CAP), pl.ds(cols, HALF)],
                        q_buf.at[d, pl.ds(CAP * k, CAP), :],
                        bsend_sem.at[j], brecv_sem.at[d], at(dy=-k, core=core),
                    )
                )
        return copies

    def back_own_copy(j):
        d = jnp.where(r == 0, j, ZN - 1 - j)
        return remote(
            o_buf.at[j, pl.ds(0, CAP), pl.ds(other, HALF)], q_buf.at[d, pl.ds(0, CAP), :],
            bsend0_sem.at[j], brecv0_sem.at[d], partner,
        )

    def give_back(j):
        d = jnp.where(r == 0, j, ZN - 1 - j)
        for copy in back_copies(j):
            copy.start()
        back_own_copy(j).start()
        q_buf[d, pl.ds(0, CAP), :] = o_buf[j, pl.ds(0, CAP), pl.ds(half, HALF)]

    def shared_copies():
        copies = []
        for k in range(XN):
            for crel, (cols, core) in enumerate(((half, r), (other, 1 - r))):
                if k or crel:
                    copies.append(
                        remote(
                            sh_buf.at[k, :, pl.ds(cols, HALF)], s_in.at[2 * k + crel - 1],
                            ssend_sem.at[2 * k + crel - 1], srecv_sem.at[0], at(dx=-k, core=core),
                        )
                    )
        return copies

    def shared():
        for k in range(1, XN):
            x_copy(k).wait_recv()
        for k in range(XN):
            gate_value = jnp.dot(t_buf[k], sgu[:, :SF], preferred_element_type=F32)
            up_value = jnp.dot(t_buf[k], sgu[:, SF:], preferred_element_type=F32)
            h_buf[pl.ds(0, TOK), pl.ds(0, SF)] = (jax.nn.silu(gate_value) * up_value).astype(BF16)

            def down_step(n, carry):
                cols = pl.ds(pl.multiple_of(n * 256, 256), 256)
                sh_buf[k, :, cols] = jnp.dot(
                    h_buf[pl.ds(0, TOK), pl.ds(0, SF)], sd[:, cols], preferred_element_type=F32
                ).astype(BF16)
                return carry

            lax.fori_loop(0, D // 256, down_step, 0)
        for copy in shared_copies():
            copy.start()

    def combined(d):
        await_bytes(q_buf.at[d, pl.ds(CAP, 3 * CAP), :], brecv_sem.at[d])

        @pl.when(r != owner(d))
        def _():
            await_bytes(q_buf.at[d, pl.ds(0, CAP), :], brecv0_sem.at[d])

        spread = jnp.concatenate([jnp.where(hit, scale, 0.0) for hit, scale in slot_parts(d)], axis=0).astype(BF16)
        return [
            lax.dot_general(
                spread, q_buf[d, :, pl.ds(part * QUARTER, QUARTER)], (((0,), (0,)), ((), ())),
                preferred_element_type=F32,
            )
            for part in range(2)
        ]

    def r_copy(way, step):
        outgoing, incoming = (plus_out, plus_in) if way == 0 else (minus_out, minus_in)
        if step == 0:
            cols = pl.ds(way * QUARTER, QUARTER)
            src, dst = outgoing.at[0, :, cols], incoming.at[0, :, cols]
        else:
            src, dst = outgoing.at[step], incoming.at[step]
        return remote(
            src, dst, rsend_sem.at[way, step], rrecv_sem.at[way, step], at(dz=1 if way == 0 else -1)
        )

    for copy in weight_copies():
        copy.start()
    dispatch(0)
    for k in range(1, XN):
        x_copy(k).start()
    z_arrived(1)
    dispatch(1)
    dispatch(7)
    for i in range(3):
        pltpu.make_async_copy(loads[i][0], loads[i][1], load_sem.at[i]).wait()
    for copy in weight_copies():
        copy.wait_recv()
    z_arrived(2)
    dispatch(2)
    dispatch(6)
    experts(0)
    z_arrived(3)
    dispatch(3)
    dispatch(5)
    z_arrived(4)
    dispatch(4)
    experts(1)
    for i in range(3, 6):
        pltpu.make_async_copy(loads[i][0], loads[i][1], load_sem.at[i]).wait()
    shared()
    experts(2)
    experts(3)
    for j in (3, 2, 1, 0):
        give_back(j)

    lo, hi = combined(4)
    plus_out[0, :, pl.ds(0, QUARTER)] = lo.astype(BF16)
    r_copy(0, 0).start()
    minus_out[0, :, pl.ds(QUARTER, QUARTER)] = hi.astype(BF16)
    r_copy(1, 0).start()
    for step in range(1, 4):
        for way in range(2):
            d = 4 - step if way == 0 else 4 + step
            outgoing, incoming = (plus_out, plus_in) if way == 0 else (minus_out, minus_in)
            sums = combined(d)
            r_copy(way, step - 1).wait_recv()
            for part in range(2):
                cols = pl.ds(part * QUARTER, QUARTER)
                if step > 1 or part == way:
                    total = sums[part] + incoming[step - 1, :, cols].astype(F32)
                else:
                    total = sums[part]
                outgoing[step, :, cols] = total.astype(BF16)
            r_copy(way, step).start()

    sums = combined(0)
    await_bytes(s_in, srecv_sem.at[0])
    r_copy(0, 3).wait_recv()
    r_copy(1, 3).wait_recv()
    for part in range(2):
        cols = pl.ds(part * QUARTER, QUARTER)
        total = sh_buf[0, :, pl.ds(pl.multiple_of(half + part * QUARTER, 128), QUARTER)].astype(F32)
        for i in range(2 * XN - 1):
            total = total + s_in[i, :, cols].astype(F32)
        total = total + sums[part] + plus_in[3, :, cols].astype(F32) + minus_in[3, :, cols].astype(F32)
        out[:, cols] = total.astype(BF16)

    for copy in weight_copies():
        copy.wait_send()
    for k in range(1, XN):
        x_copy(k).wait_send()
    for way in range(2):
        for k in range(1, ZN // 2 + 1):
            for copy in z_copies(way, k):
                copy.wait_send()
        for step in range(4):
            r_copy(way, step).wait_send()
    for d in range(ZN):
        await_bytes(d_buf.at[d, pl.ds(CAP, 3 * CAP), :], ysend_sem.at[d])

        @pl.when(r != owner(d))
        def _():
            y_own_copy(d).wait_send()

    for j in range(ZN // 2):
        await_bytes(o_buf.at[j, pl.ds(CAP, 3 * CAP), :], bsend_sem.at[j])
        back_own_copy(j).wait_send()
    for copy in shared_copies():
        copy.wait_send()


def on_device(*args):
    tokens, norm_gain, *rest = args
    vmem = pl.BlockSpec(memory_space=pltpu.VMEM)
    hbm = pl.BlockSpec(memory_space=pl.ANY)
    dma = lambda *shape: pltpu.SemaphoreType.DMA(shape)
    half_z = ZN // 2
    return pl.pallas_call(
        kernel,
        out_shape=jax.ShapeDtypeStruct((TOK, HALF), BF16),
        in_specs=[vmem] * 4 + [hbm] * 6,
        out_specs=vmem,
        scratch_shapes=[
            pltpu.VMEM((XN, TOK, D), BF16),
            pltpu.VMEM((ZN, TOK, HALF), BF16),
            pltpu.VMEM((ZN, EXPERTS, TOK), F32),
            pltpu.VMEM((ZN, ROWS, HALF), BF16),
            pltpu.VMEM((half_z, ROWS, D), BF16),
            pltpu.VMEM((ROWS, FF), BF16),
            pltpu.VMEM((half_z, ROWS, D), BF16),
            pltpu.VMEM((ZN, ROWS, HALF), BF16),
            pltpu.VMEM((4, TOK, HALF), BF16),
            pltpu.VMEM((4, TOK, HALF), BF16),
            pltpu.VMEM((4, TOK, HALF), BF16),
            pltpu.VMEM((4, TOK, HALF), BF16),
            pltpu.VMEM((XN, TOK, D), BF16),
            pltpu.VMEM((2 * XN - 1, TOK, HALF), BF16),
            pltpu.VMEM((D, FF), BF16),
            pltpu.VMEM((D, FF), BF16),
            pltpu.VMEM((FF, D), BF16),
            pltpu.VMEM((D, 2 * SF), BF16),
            pltpu.VMEM((SF, D), BF16),
            dma(6), dma(3), dma(3),
            dma(2, 4), dma(2, 4), dma(2, 4), dma(2, 4),
            dma(ZN), dma(half_z), dma(ZN), dma(half_z),
            dma(half_z), dma(ZN), dma(half_z), dma(ZN),
            dma(2, 4), dma(2, 4),
            dma(3), dma(3), dma(2 * XN - 1), dma(1),
        ],
        compiler_params=pltpu.CompilerParams(
            collective_id=0, has_side_effects=True, vmem_limit_bytes=63 * 2**20
        ),
    )(tokens, norm_gain.reshape(1, D), *rest)


def solution(mesh):
    placed = (
        P(("dp", "expert"), None),
        P(),
        P(("dp", "expert"), None),
        P(("dp", "expert"), None),
        P("expert", None, "tensor"),
        P("expert", None, "tensor"),
        P("expert", "tensor", None),
        P(None, ("dp", "tensor")),
        P(None, ("dp", "tensor")),
        P(("dp", "tensor"), None),
    )
    return jax.shard_map(
        on_device,
        mesh=mesh,
        in_specs=placed,
        out_specs=P(("dp", "expert"), "tensor"),
        check_vma=False,
    )
```

```python
import jax
import jax.numpy as jnp
from jax import lax
from jax.experimental import pallas as pl
from jax.experimental.pallas import tpu as pltpu
from jax.sharding import PartitionSpec as P

D = 2560
HALF = D // 2
QUARTER = HALF // 2
FF2 = 384
FF = 768
SF = 256
EXPERTS = 32
TOP = 6
TOK = 128
CAP = 48
YN = 4
ZN = 8
XN = 4
ROWS = YN * CAP
EPSILON = 1e-06
MESH = pl.DeviceIdType.MESH
BF16 = jnp.bfloat16
F32 = jnp.float32


def owner(d):
    return 0 if d < ZN // 2 else 1


def chunk_of(d):
    return d if d < ZN // 2 else ZN - 1 - d


def kernel(
    tokens, gain, ids, weights, wg_in, wu_in, wd_in, sg_in, su_in, sd_in,
    out,
    t_buf, g_buf, code, d_buf, r_buf, h_buf, o_buf, q_buf,
    plus_in, minus_in, plus_out, minus_out, sh_hidden, sh_buf, s_in,
    wg, wu, wd, sgu, sd,
    load_sem, wsend_sem, wrecv_sem,
    zsend_sem, zrecv_sem, csend_sem, crecv_sem,
    ysend_sem, yrecv_sem, ysend0_sem, yrecv0_sem,
    bsend_sem, brecv_sem, bsend0_sem, brecv0_sem,
    rsend_sem, rrecv_sem,
    xsend_sem, xrecv_sem, ssend_sem, srecv_sem,
):
    x = lax.axis_index("dp")
    e = lax.axis_index("expert")
    r = lax.axis_index("tensor")
    y = e // ZN
    z = e % ZN
    half = pl.multiple_of(r * HALF, 128)
    other = pl.multiple_of((1 - r) * HALF, 128)

    def at(dx=0, dy=0, dz=0, core=None):
        return (
            (x + dx + XN) % XN,
            ((y + dy + YN) % YN) * ZN + (z + dz + ZN) % ZN,
            r if core is None else core,
        )

    partner = at(core=1 - r)

    def remote(src, dst, send, recv, device):
        return pltpu.make_async_remote_copy(
            src_ref=src, dst_ref=dst, send_sem=send, recv_sem=recv,
            device_id=device, device_id_type=MESH,
        )

    def await_bytes(ref, sem):
        pltpu.make_async_copy(ref, ref, sem).wait()

    barrier = pltpu.get_barrier_semaphore()
    peers = [partner, at(dz=1), at(dz=-1)]
    for k in range(1, YN):
        peers += [at(dy=k), at(dy=k, core=1 - r)]
    for k in range(1, XN):
        peers += [at(dx=k), at(dx=k, core=1 - r)]
    for peer in peers:
        pl.semaphore_signal(barrier, inc=1, device_id=peer, device_id_type=MESH)

    loads = [
        (wg_in.at[0], wg.at[:, pl.ds(0, FF2)]),
        (wu_in.at[0], wu.at[:, pl.ds(0, FF2)]),
        (wd_in.at[0], wd.at[pl.ds(0, FF2), :]),
        (sg_in, sgu.at[:, pl.ds(0, SF)]),
        (su_in, sgu.at[:, pl.ds(SF, SF)]),
        (sd_in, sd),
    ]
    for i, (src, dst) in enumerate(loads):
        pltpu.make_async_copy(src, dst, load_sem.at[i]).start()

    gain_row = gain[...].reshape(1, D)

    def norm_step(i, carry):
        rows = pl.ds(pl.multiple_of(i * 16, 16), 16)
        values = tokens[rows, :].astype(F32)
        inverse = lax.rsqrt(jnp.mean(values * values, axis=1, keepdims=True) + EPSILON)
        normed = values * inverse * gain_row
        t_buf[rows, :] = normed.astype(BF16)
        g_buf[0, rows, :] = jnp.where(r == 0, normed[:, :HALF], normed[:, HALF:]).astype(BF16)
        return carry

    lax.fori_loop(0, TOK // 16, norm_step, 0)

    expert_row = lax.broadcasted_iota(jnp.int32, (EXPERTS, TOK), 0)
    named = jnp.zeros((EXPERTS, TOK), F32)
    weight = jnp.zeros((EXPERTS, TOK), F32)
    for k in range(TOP):
        match = ids[k : k + 1, :] == expert_row
        named = jnp.where(match, 1.0, named)
        weight = jnp.where(match, weights[k : k + 1, :].astype(F32), weight)
    before = lax.broadcasted_iota(jnp.int32, (TOK, TOK), 0) < lax.broadcasted_iota(jnp.int32, (TOK, TOK), 1)
    earlier = jnp.where(before, 1.0, 0.0).astype(BF16)
    rank = jnp.dot(named.astype(BF16), earlier, preferred_element_type=F32)
    code[0] = jnp.where(named > 0.5, weight * 64.0 + rank, -1.0)

    pl.semaphore_wait(barrier, len(peers))

    def z_pieces(k):
        return [(way, part) for part in range(2) for way in range(2) if k < ZN // 2 or way == part]

    def z_copies(k, way, part):
        if way == 0:
            here, there, to = k - 1, k, at(dz=-1)
        else:
            here, there, to = (ZN - (k - 1)) % ZN, ZN - k, at(dz=1)
        cols = pl.ds(part * QUARTER, QUARTER)
        copies = [
            remote(
                g_buf.at[here, :, cols], g_buf.at[there, :, cols],
                zsend_sem.at[way, part, k - 1], zrecv_sem.at[way, part, k - 1], to,
            )
        ]
        if part == 0 and (k < ZN // 2 or way == 0):
            copies.append(
                remote(code.at[here], code.at[there], csend_sem.at[way, k - 1], crecv_sem.at[way, k - 1], to)
            )
        return copies

    def weight_copies():
        return [
            remote(wg_in.at[0], wg.at[:, pl.ds(FF2, FF2)], wsend_sem.at[0], wrecv_sem.at[0], partner),
            remote(wu_in.at[0], wu.at[:, pl.ds(FF2, FF2)], wsend_sem.at[1], wrecv_sem.at[1], partner),
            remote(wd_in.at[0], wd.at[pl.ds(FF2, FF2), :], wsend_sem.at[2], wrecv_sem.at[2], partner),
        ]

    def x_copy(k):
        return remote(t_buf.at[pl.ds(0, TOK)], t_buf.at[pl.ds(TOK * k, TOK)], xsend_sem.at[k - 1], xrecv_sem.at[k - 1], at(dx=k))

    for piece in z_pieces(1):
        for copy in z_copies(1, *piece):
            copy.start()

    slot = lax.broadcasted_iota(jnp.int32, (CAP, TOK), 0).astype(F32)

    def slot_parts(d):
        for k in range(YN):
            expert = ((y + k) % YN) * ZN + z
            line = code[d, pl.ds(expert, 1), :]
            scale = jnp.floor(line * (1.0 / 64.0))
            yield slot == line - 64.0 * scale, scale * (1.0 / 64.0)

    def y_copies(d):
        j, core = chunk_of(d), owner(d)
        return [
            remote(
                d_buf.at[d, pl.ds(CAP * k, CAP), :],
                r_buf.at[pl.ds(ROWS * j + CAP * k, CAP), pl.ds(half, HALF)],
                ysend_sem.at[d], yrecv_sem.at[j], at(dy=k, core=core),
            )
            for k in range(1, YN)
        ]

    def y_own_copy(d):
        return remote(
            d_buf.at[d, pl.ds(0, CAP), :],
            r_buf.at[pl.ds(ROWS * chunk_of(d), CAP), pl.ds(half, HALF)],
            ysend0_sem.at[d], yrecv0_sem.at[chunk_of(d)], partner,
        )

    def dispatch(d):
        pick = jnp.concatenate([jnp.where(hit, 1.0, 0.0) for hit, _ in slot_parts(d)], axis=0).astype(BF16)
        for cols in (pl.ds(0, QUARTER), pl.ds(QUARTER, QUARTER)):
            d_buf[d, :, cols] = jnp.dot(pick, g_buf[d, :, cols], preferred_element_type=F32).astype(BF16)
        for copy in y_copies(d):
            copy.start()

        @pl.when(r == owner(d))
        def _():
            r_buf[pl.ds(ROWS * chunk_of(d), CAP), pl.ds(half, HALF)] = d_buf[d, pl.ds(0, CAP), :]

        @pl.when(r != owner(d))
        def _():
            y_own_copy(d).start()

    def z_arrived(k):
        for piece in z_pieces(k):
            for copy in z_copies(k, *piece):
                copy.wait_recv()
            if k < ZN // 2 and piece in z_pieces(k + 1):
                for copy in z_copies(k + 1, *piece):
                    copy.start()

    def experts(*chunks):
        for j in chunks:
            await_bytes(r_buf.at[pl.ds(ROWS * j + CAP, 3 * CAP), :], yrecv_sem.at[j])
            await_bytes(r_buf.at[pl.ds(ROWS * j, CAP), pl.ds(other, HALF)], yrecv0_sem.at[j])
        rows = pl.ds(ROWS * chunks[0], ROWS * len(chunks))
        top = pl.ds(0, ROWS * len(chunks))

        def up_step(n, carry):
            cols = pl.ds(pl.multiple_of(n * 256, 256), 256)
            gate_value = jnp.dot(r_buf[rows, :], wg[:, cols], preferred_element_type=F32)
            up_value = jnp.dot(r_buf[rows, :], wu[:, cols], preferred_element_type=F32)
            h_buf[top, cols] = (jax.nn.silu(gate_value) * up_value).astype(BF16)
            return carry

        lax.fori_loop(0, FF // 256, up_step, 0)

        def down_step(n, carry):
            cols = pl.ds(pl.multiple_of(n * 256, 256), 256)
            o_buf[rows, cols] = jnp.dot(h_buf[top, :], wd[:, cols], preferred_element_type=F32).astype(BF16)
            return carry

        lax.fori_loop(0, D // 256, down_step, 0)

    def back_copies(j):
        d = jnp.where(r == 0, j, ZN - 1 - j)
        copies = []
        for k in range(1, YN):
            for cols, core in ((half, r), (other, 1 - r)):
                copies.append(
                    remote(
                        o_buf.at[pl.ds(ROWS * j + CAP * k, CAP), pl.ds(cols, HALF)],
                        q_buf.at[d, pl.ds(CAP * k, CAP), :],
                        bsend_sem.at[j], brecv_sem.at[d], at(dy=-k, core=core),
                    )
                )
        return copies

    def back_own_copy(j):
        d = jnp.where(r == 0, j, ZN - 1 - j)
        return remote(
            o_buf.at[pl.ds(ROWS * j, CAP), pl.ds(other, HALF)], q_buf.at[d, pl.ds(0, CAP), :],
            bsend0_sem.at[j], brecv0_sem.at[d], partner,
        )

    def give_back(j):
        d = jnp.where(r == 0, j, ZN - 1 - j)
        for copy in back_copies(j):
            copy.start()
        back_own_copy(j).start()
        q_buf[d, pl.ds(0, CAP), :] = o_buf[pl.ds(ROWS * j, CAP), pl.ds(half, HALF)]

    def shared_copies():
        copies = []
        for k in range(XN):
            for crel, (cols, core) in enumerate(((half, r), (other, 1 - r))):
                if k or crel:
                    copies.append(
                        remote(
                            sh_buf.at[pl.ds(TOK * k, TOK), pl.ds(cols, HALF)], s_in.at[2 * k + crel - 1],
                            ssend_sem.at[2 * k + crel - 1], srecv_sem.at[0], at(dx=-k, core=core),
                        )
                    )
        return copies

    def shared():
        for k in range(1, XN):
            x_copy(k).wait_recv()
        gate_value = jnp.dot(t_buf[...], sgu[:, :SF], preferred_element_type=F32)
        up_value = jnp.dot(t_buf[...], sgu[:, SF:], preferred_element_type=F32)
        sh_hidden[...] = (jax.nn.silu(gate_value) * up_value).astype(BF16)

        def down_step(n, carry):
            cols = pl.ds(pl.multiple_of(n * 256, 256), 256)
            sh_buf[:, cols] = jnp.dot(sh_hidden[...], sd[:, cols], preferred_element_type=F32).astype(BF16)
            return carry

        lax.fori_loop(0, D // 256, down_step, 0)
        for copy in shared_copies():
            copy.start()

    def combined(d):
        await_bytes(q_buf.at[d, pl.ds(CAP, 3 * CAP), :], brecv_sem.at[d])

        @pl.when(r != owner(d))
        def _():
            await_bytes(q_buf.at[d, pl.ds(0, CAP), :], brecv0_sem.at[d])

        spread = jnp.concatenate([jnp.where(hit, scale, 0.0) for hit, scale in slot_parts(d)], axis=0).astype(BF16)
        return [
            lax.dot_general(
                spread, q_buf[d, :, pl.ds(part * QUARTER, QUARTER)], (((0,), (0,)), ((), ())),
                preferred_element_type=F32,
            )
            for part in range(2)
        ]

    def r_copy(step, way, part):
        outgoing, incoming = (plus_out, plus_in) if way == 0 else (minus_out, minus_in)
        cols = pl.ds(part * QUARTER, QUARTER)
        return remote(
            outgoing.at[step, :, cols], incoming.at[step, :, cols],
            rsend_sem.at[way, part, step], rrecv_sem.at[way, part, step], at(dz=1 if way == 0 else -1),
        )

    for copy in weight_copies():
        copy.start()
    dispatch(0)
    for k in range(1, XN):
        x_copy(k).start()
    z_arrived(1)
    dispatch(1)
    dispatch(7)
    z_arrived(2)
    dispatch(2)
    dispatch(6)
    z_arrived(3)
    dispatch(3)
    dispatch(5)
    z_arrived(4)
    dispatch(4)
    for i in range(3):
        pltpu.make_async_copy(loads[i][0], loads[i][1], load_sem.at[i]).wait()
    for copy in weight_copies():
        copy.wait_recv()
    experts(0, 1)
    for i in range(3, 6):
        pltpu.make_async_copy(loads[i][0], loads[i][1], load_sem.at[i]).wait()
    shared()
    experts(2)
    give_back(2)
    experts(3)
    give_back(3)
    give_back(1)
    give_back(0)

    sums = combined(4)
    for way in range(2):
        outgoing = plus_out if way == 0 else minus_out
        outgoing[0, :, pl.ds(way * QUARTER, QUARTER)] = sums[way].astype(BF16)
        r_copy(0, way, way).start()
    for step in range(1, 4):
        both = [combined(4 - step), combined(4 + step)]
        for i in range(2):
            for way in range(2):
                part = 1 - i if way == 0 else i
                outgoing, incoming = (plus_out, plus_in) if way == 0 else (minus_out, minus_in)
                cols = pl.ds(part * QUARTER, QUARTER)
                total = both[way][part]
                if step > 1 or part == way:
                    r_copy(step - 1, way, part).wait_recv()
                    total = total + incoming[step - 1, :, cols].astype(F32)
                outgoing[step, :, cols] = total.astype(BF16)
                r_copy(step, way, part).start()

    sums = combined(0)
    await_bytes(s_in, srecv_sem.at[0])
    for part in range(2):
        cols = pl.ds(part * QUARTER, QUARTER)
        total = sh_buf[pl.ds(0, TOK), pl.ds(pl.multiple_of(half + part * QUARTER, 128), QUARTER)].astype(F32)
        for i in range(2 * XN - 1):
            total = total + s_in[i, :, cols].astype(F32)
        both[part] = total + sums[part]
    for way, part in ((0, 1), (1, 0), (0, 0), (1, 1)):
        r_copy(3, way, part).wait_recv()
        incoming = plus_in if way == 0 else minus_in
        both[part] = both[part] + incoming[3, :, pl.ds(part * QUARTER, QUARTER)].astype(F32)
    for part in range(2):
        out[:, pl.ds(part * QUARTER, QUARTER)] = both[part].astype(BF16)

    for copy in weight_copies():
        copy.wait_send()
    for k in range(1, XN):
        x_copy(k).wait_send()
    for k in range(1, ZN // 2 + 1):
        for piece in z_pieces(k):
            for copy in z_copies(k, *piece):
                copy.wait_send()
    for step in range(4):
        for piece in z_pieces(4 - step):
            r_copy(step, *piece).wait_send()
    for d in range(ZN):
        await_bytes(d_buf.at[d, pl.ds(CAP, 3 * CAP), :], ysend_sem.at[d])

        @pl.when(r != owner(d))
        def _():
            y_own_copy(d).wait_send()

    for j in range(ZN // 2):
        await_bytes(o_buf.at[pl.ds(ROWS * j + CAP, 3 * CAP), :], bsend_sem.at[j])
        back_own_copy(j).wait_send()
    for copy in shared_copies():
        copy.wait_send()


def on_device(*args):
    tokens, norm_gain, expert_ids, route_weights, *rest = args
    vmem = pl.BlockSpec(memory_space=pltpu.VMEM)
    hbm = pl.BlockSpec(memory_space=pl.ANY)
    dma = lambda *shape: pltpu.SemaphoreType.DMA(shape)
    half_z = ZN // 2
    return pl.pallas_call(
        kernel,
        out_shape=jax.ShapeDtypeStruct((TOK, HALF), BF16),
        in_specs=[vmem] * 4 + [hbm] * 6,
        out_specs=vmem,
        scratch_shapes=[
            pltpu.VMEM((XN * TOK, D), BF16),
            pltpu.VMEM((ZN, TOK, HALF), BF16),
            pltpu.VMEM((ZN, EXPERTS, TOK), F32),
            pltpu.VMEM((ZN, ROWS, HALF), BF16),
            pltpu.VMEM((half_z * ROWS, D), BF16),
            pltpu.VMEM((2 * ROWS, FF), BF16),
            pltpu.VMEM((half_z * ROWS, D), BF16),
            pltpu.VMEM((ZN, ROWS, HALF), BF16),
            pltpu.VMEM((4, TOK, HALF), BF16),
            pltpu.VMEM((4, TOK, HALF), BF16),
            pltpu.VMEM((4, TOK, HALF), BF16),
            pltpu.VMEM((4, TOK, HALF), BF16),
            pltpu.VMEM((XN * TOK, SF), BF16),
            pltpu.VMEM((XN * TOK, D), BF16),
            pltpu.VMEM((2 * XN - 1, TOK, HALF), BF16),
            pltpu.VMEM((D, FF), BF16),
            pltpu.VMEM((D, FF), BF16),
            pltpu.VMEM((FF, D), BF16),
            pltpu.VMEM((D, 2 * SF), BF16),
            pltpu.VMEM((SF, D), BF16),
            dma(6), dma(3), dma(3),
            dma(2, 2, 4), dma(2, 2, 4), dma(2, 4), dma(2, 4),
            dma(ZN), dma(half_z), dma(ZN), dma(half_z),
            dma(half_z), dma(ZN), dma(half_z), dma(ZN),
            dma(2, 2, 4), dma(2, 2, 4),
            dma(3), dma(3), dma(2 * XN - 1), dma(1),
        ],
        compiler_params=pltpu.CompilerParams(
            collective_id=0, has_side_effects=True, vmem_limit_bytes=63 * 2**20
        ),
    )(tokens, norm_gain, expert_ids.T, route_weights.T, *rest)


def solution(mesh):
    placed = (
        P(("dp", "expert"), None),
        P(),
        P(("dp", "expert"), None),
        P(("dp", "expert"), None),
        P("expert", None, "tensor"),
        P("expert", None, "tensor"),
        P("expert", "tensor", None),
        P(None, ("dp", "tensor")),
        P(None, ("dp", "tensor")),
        P(("dp", "tensor"), None),
    )
    return jax.shard_map(
        on_device,
        mesh=mesh,
        in_specs=placed,
        out_specs=P(("dp", "expert"), "tensor"),
        check_vma=False,
    )
```

```python
import jax
import jax.numpy as jnp
from jax import lax
from jax.experimental import pallas as pl
from jax.experimental.pallas import tpu as pltpu
from jax.sharding import PartitionSpec as P

D = 2560
HALF = D // 2
QUARTER = HALF // 2
FF2 = 384
FF = 768
SF = 256
EXPERTS = 32
TOP = 6
TOK = 128
CAP = 48
YN = 4
ZN = 8
XN = 4
ROWS = YN * CAP
EPSILON = 1e-06
MESH = pl.DeviceIdType.MESH
ORDER = (0, 1, 3, 2)
PLACE = {k: CAP * ORDER.index(k) for k in ORDER}
FAR = (0, 7, 1, 4, 6, 2, 5, 3)
NEAR = FAR[:4]
BF16 = jnp.bfloat16
F32 = jnp.float32


def owner(d):
    return 0 if d < ZN // 2 else 1


def signed(d):
    return d if d <= ZN // 2 else d - ZN


def along_y(d):
    return (1, 3) if d in NEAR else (1, 3, 2)


def back_along_y(d):
    return (1, 3) if d in FAR else (1, 3, 2)


def chunk_of(d):
    return d if d < ZN // 2 else ZN - 1 - d


def kernel(
    tokens, gain, ids, weights, wg_in, wu_in, wd_in, sg_in, su_in, sd_in,
    out,
    t_buf, g_buf, code, d_buf, r_buf, h_buf, o_buf, q_buf,
    far_tok, far_code, far_rows, far_q, far_out, far_in,
    plus_in, minus_in, plus_out, minus_out, sh_hidden, sh_buf, s_in,
    wgu, wd, sgu, sd,
    load_sem, wsend_sem, wrecv_sem,
    zsend_sem, zrecv_sem, csend_sem, crecv_sem,
    ysend_sem, yrecv_sem, ysend0_sem, yrecv0_sem,
    bsend_sem, brecv_sem, bsend0_sem, brecv0_sem,
    rsend_sem, rrecv_sem,
    xsend_sem, xrecv_sem, ssend_sem, srecv_sem,
    fsend_sem, frecv_sem, fdsend_sem, fdrecv_sem, fbsend_sem, fbrecv_sem,
):
    x = lax.axis_index("dp")
    e = lax.axis_index("expert")
    r = lax.axis_index("tensor")
    y = e // ZN
    z = e % ZN
    half = pl.multiple_of(r * HALF, 128)
    other = pl.multiple_of((1 - r) * HALF, 128)

    def at(dx=0, dy=0, dz=0, core=None):
        return (
            (x + dx + XN) % XN,
            ((y + dy + YN) % YN) * ZN + (z + dz + ZN) % ZN,
            r if core is None else core,
        )

    partner = at(core=1 - r)
    here_rows = pl.multiple_of(r * (TOK // 2), TOK // 2)
    other_rows = pl.multiple_of((1 - r) * (TOK // 2), TOK // 2)

    def remote(src, dst, send, recv, device):
        return pltpu.make_async_remote_copy(
            src_ref=src, dst_ref=dst, send_sem=send, recv_sem=recv,
            device_id=device, device_id_type=MESH,
        )

    def await_bytes(ref, sem):
        pltpu.make_async_copy(ref, ref, sem).wait()

    barrier = pltpu.get_barrier_semaphore()
    peers = [partner]
    for k in range(1, ZN):
        peers += [at(dz=k), at(dz=k, core=1 - r)]
    for k in range(1, YN):
        peers += [at(dy=k), at(dy=k, core=1 - r)]
    for k in range(1, XN):
        peers += [at(dx=k), at(dx=k, core=1 - r)]
    for peer in peers:
        pl.semaphore_signal(barrier, inc=1, device_id=peer, device_id_type=MESH)

    loads = [
        (wg_in.at[0], wgu.at[:, pl.ds(0, FF2)]),
        (wu_in.at[0], wgu.at[:, pl.ds(FF, FF2)]),
        (wd_in.at[0], wd.at[pl.ds(0, FF2), :]),
        (sg_in, sgu.at[:, pl.ds(0, SF)]),
        (su_in, sgu.at[:, pl.ds(2 * SF, SF)]),
        (sd_in, sd.at[pl.ds(0, SF), :]),
    ]
    for i, (src, dst) in enumerate(loads):
        pltpu.make_async_copy(src, dst, load_sem.at[i]).start()

    gain_row = gain[...].reshape(1, D)

    def norm_step(i, carry):
        rows = pl.ds(pl.multiple_of(i * 16, 16), 16)
        values = tokens[rows, :].astype(F32)
        inverse = lax.rsqrt(jnp.mean(values * values, axis=1, keepdims=True) + EPSILON)
        normed = values * inverse * gain_row
        @pl.when(i // 4 == r)
        def _():
            t_buf[pl.ds(pl.multiple_of((i % 4) * 16, 16), 16), :] = normed.astype(BF16)

        g_buf[0, rows, :] = jnp.where(r == 0, normed[:, :HALF], normed[:, HALF:]).astype(BF16)
        return carry

    lax.fori_loop(0, TOK // 16, norm_step, 0)

    expert_row = lax.broadcasted_iota(jnp.int32, (EXPERTS, TOK), 0)
    named = jnp.zeros((EXPERTS, TOK), F32)
    weight = jnp.zeros((EXPERTS, TOK), F32)
    for k in range(TOP):
        match = ids[k : k + 1, :] == expert_row
        named = jnp.where(match, 1.0, named)
        weight = jnp.where(match, weights[k : k + 1, :].astype(F32), weight)
    before = lax.broadcasted_iota(jnp.int32, (TOK, TOK), 0) < lax.broadcasted_iota(jnp.int32, (TOK, TOK), 1)
    earlier = jnp.where(before, 1.0, 0.0).astype(BF16)
    rank = jnp.dot(named.astype(BF16), earlier, preferred_element_type=F32)
    code[0] = jnp.where(named > 0.5, weight * 64.0 + rank, -1.0)

    pl.semaphore_wait(barrier, len(peers))

    def z_pieces(k):
        return [(way, part) for part in range(2) for way in range(2) if k < ZN // 2 or way == part]

    def z_copies(k, way, part):
        if way == 0:
            here, there, to = k - 1, k, at(dz=-1)
        else:
            here, there, to = (ZN - (k - 1)) % ZN, ZN - k, at(dz=1)
        cols = pl.ds(part * QUARTER, QUARTER)
        copies = [
            remote(
                g_buf.at[here, :, cols], g_buf.at[there, :, cols],
                zsend_sem.at[way, part, k - 1], zrecv_sem.at[way, part, k - 1], to,
            )
        ]
        if part == 0 and (k < ZN // 2 or way == 0):
            copies.append(
                remote(code.at[here], code.at[there], csend_sem.at[way, k - 1], crecv_sem.at[way, k - 1], to)
            )
        return copies

    partner_places = [
        wgu.at[:, pl.ds(FF2, FF2)],
        wgu.at[:, pl.ds(FF + FF2, FF2)],
        wd.at[pl.ds(FF2, FF2), :],
        sgu.at[:, pl.ds(SF, SF)],
        sgu.at[:, pl.ds(3 * SF, SF)],
        sd.at[pl.ds(SF, SF), :],
    ]

    def weight_copy(i):
        return remote(loads[i][0], partner_places[i], wsend_sem.at[i], wrecv_sem.at[i], partner)

    def x_copy(k):
        return remote(t_buf.at[pl.ds(0, TOK // 2)], t_buf.at[pl.ds(TOK // 2 * k, TOK // 2)], xsend_sem.at[k - 1], xrecv_sem.at[k - 1], at(dx=k))

    for piece in z_pieces(1):
        for copy in z_copies(1, *piece):
            copy.start()

    slot = lax.broadcasted_iota(jnp.int32, (CAP, TOK), 0).astype(F32)

    def slot_parts(line_of, experts):
        for expert in experts:
            line = line_of(expert)
            scale = jnp.floor(line * (1.0 / 64.0))
            yield slot == line - 64.0 * scale, scale * (1.0 / 64.0)

    def picks(line_of, experts):
        return jnp.concatenate(
            [jnp.where(hit, 1.0, 0.0) for hit, _ in slot_parts(line_of, experts)], axis=0
        ).astype(BF16)

    def spreads(line_of, experts):
        return jnp.concatenate(
            [jnp.where(hit, scale, 0.0) for hit, scale in slot_parts(line_of, experts)], axis=0
        ).astype(BF16)

    def expert_at(dy=0, dz=0):
        return ((y + dy + YN) % YN) * ZN + (z + dz + ZN) % ZN

    def y_experts(d):
        return [expert_at(dy=k) for k in ORDER if k == 0 or k in along_y(d)]

    def y_copies(d):
        j, core = chunk_of(d), owner(d)
        return [
            remote(
                d_buf.at[d, pl.ds(PLACE[k], CAP), :],
                r_buf.at[pl.ds(ROWS * j + PLACE[k], CAP), pl.ds(half, HALF)],
                ysend_sem.at[d], yrecv_sem.at[j], at(dy=k, core=core),
            )
            for k in along_y(d)
        ]

    def y_own_copy(d):
        return remote(
            d_buf.at[d, pl.ds(0, CAP), :],
            r_buf.at[pl.ds(ROWS * chunk_of(d), CAP), pl.ds(half, HALF)],
            ysend0_sem.at[d], yrecv0_sem.at[chunk_of(d)], partner,
        )

    def dispatch(d):
        pick = picks(lambda expert: code[d, pl.ds(expert, 1), :], y_experts(d))
        rows = pl.ds(0, CAP * (1 + len(along_y(d))))
        for cols in (pl.ds(0, QUARTER), pl.ds(QUARTER, QUARTER)):
            d_buf[d, rows, cols] = jnp.dot(pick, g_buf[d, :, cols], preferred_element_type=F32).astype(BF16)
        for copy in y_copies(d):
            copy.start()

        @pl.when(r == owner(d))
        def _():
            r_buf[pl.ds(ROWS * chunk_of(d), CAP), pl.ds(half, HALF)] = d_buf[d, pl.ds(0, CAP), :]

        @pl.when(r != owner(d))
        def _():
            y_own_copy(d).start()

    def far_copies():
        return [
            remote(g_buf.at[0], far_tok, fsend_sem.at[0], frecv_sem.at[0], at(dy=2)),
            remote(code.at[0], far_code, fsend_sem.at[1], frecv_sem.at[1], at(dy=2)),
        ]

    def far_experts(distances):
        return [expert_at(dz=-signed(d)) for d in distances]

    def far_line(expert):
        return far_code[pl.ds(expert, 1), :]

    def far_row_copy(i):
        d = NEAR[i]
        j = chunk_of(d)
        return remote(
            far_rows.at[pl.ds(CAP * i, CAP), :],
            r_buf.at[pl.ds(ROWS * j + PLACE[2], CAP), pl.ds(half, HALF)],
            fdsend_sem.at[i], fdrecv_sem.at[j],
            partner if d == 0 else at(dz=-signed(d), core=owner(d)),
        )

    def far_pick():
        for copy in far_copies():
            copy.wait_recv()
        pick = picks(far_line, far_experts(NEAR))
        for cols in (pl.ds(0, QUARTER), pl.ds(QUARTER, QUARTER)):
            far_rows[:, cols] = jnp.dot(pick, far_tok[:, cols], preferred_element_type=F32).astype(BF16)

        @pl.when(r == 0)
        def _():
            r_buf[pl.ds(PLACE[2], CAP), pl.ds(half, HALF)] = far_rows[pl.ds(0, CAP), :]

        @pl.when(r == 1)
        def _():
            far_row_copy(0).start()

        for i in (1, 2):
            far_row_copy(i).start()

    def far_pick_two():
        far_row_copy(3).start()

    def z_arrived(k):
        for piece in z_pieces(k):
            for copy in z_copies(k, *piece):
                copy.wait_recv()
            if k < ZN // 2 and piece in z_pieces(k + 1):
                for copy in z_copies(k + 1, *piece):
                    copy.start()

    def experts(j):
        await_bytes(r_buf.at[pl.ds(ROWS * j, CAP), pl.ds(other, HALF)], yrecv0_sem.at[j])
        for core, d in ((0, j), (1, ZN - 1 - j)):

            @pl.when(r == core)
            def _():
                await_bytes(r_buf.at[pl.ds(ROWS * j + CAP, CAP * len(along_y(d))), :], yrecv_sem.at[j])
                if d == 0:
                    await_bytes(r_buf.at[pl.ds(ROWS * j + PLACE[2], CAP), pl.ds(other, HALF)], fdrecv_sem.at[j])
                elif d in NEAR:
                    await_bytes(r_buf.at[pl.ds(ROWS * j + PLACE[2], CAP), :], fdrecv_sem.at[j])

        rows = pl.ds(ROWS * j, ROWS)

        both = jnp.dot(r_buf[rows, :], wgu[...], preferred_element_type=F32)
        h_buf[...] = (jax.nn.silu(both[:, :FF]) * both[:, FF:]).astype(BF16)
        o_buf[rows, :] = jnp.dot(h_buf[...], wd[...], preferred_element_type=F32).astype(BF16)

    def back_copies(j, d):
        copies = []
        for k in back_along_y(d):
            for cols, core in ((half, r), (other, 1 - r)):
                copies.append(
                    remote(
                        o_buf.at[pl.ds(ROWS * j + PLACE[k], CAP), pl.ds(cols, HALF)],
                        q_buf.at[d, pl.ds(PLACE[k], CAP), :],
                        bsend_sem.at[j], brecv_sem.at[d], at(dy=-k, core=core),
                    )
                )
        return copies

    def back_own_copy(j, d):
        return remote(
            o_buf.at[pl.ds(ROWS * j, CAP), pl.ds(other, HALF)], q_buf.at[d, pl.ds(0, CAP), :],
            bsend0_sem.at[j], brecv0_sem.at[d], partner,
        )

    def far_back_copies(j, d):
        i = FAR.index(d)
        copies = []
        for cols, core in ((half, r), (other, 1 - r)):
            if d == 0 and core is r:
                continue
            copies.append(
                remote(
                    o_buf.at[pl.ds(ROWS * j + PLACE[2], CAP), pl.ds(cols, HALF)],
                    far_q.at[pl.ds(CAP * i, CAP), :],
                    fbsend_sem.at[j, 0 if core is r else 1], fbrecv_sem.at[i], at(dz=signed(d), core=core),
                )
            )
        return copies

    def give_back(j, cores=(0, 1)):
        for core in cores:
            d = j if core == 0 else ZN - 1 - j

            @pl.when(r == core)
            def _():
                for copy in back_copies(j, d):
                    copy.start()
                back_own_copy(j, d).start()
                q_buf[d, pl.ds(0, CAP), :] = o_buf[pl.ds(ROWS * j, CAP), pl.ds(half, HALF)]

    def give_far(j):
        for core, d in ((0, j), (1, ZN - 1 - j)):

            @pl.when(r == core)
            def _():
                if d in FAR:
                    for copy in far_back_copies(j, d):
                        copy.start()
                if d == 0:
                    far_q[pl.ds(0, CAP), :] = o_buf[pl.ds(PLACE[2], CAP), pl.ds(half, HALF)]

    def far_out_copy():
        return remote(far_out, far_in, fsend_sem.at[2], frecv_sem.at[2], at(dy=2))

    def far_sum():
        @pl.when(r == 1)
        def _():
            await_bytes(far_q.at[pl.ds(0, CAP), :], fbrecv_sem.at[0])

        for i in range(1, len(FAR)):
            await_bytes(far_q.at[pl.ds(CAP * i, CAP), :], fbrecv_sem.at[i])
        spread = spreads(far_line, far_experts(FAR))
        for cols in (pl.ds(0, QUARTER), pl.ds(QUARTER, QUARTER)):
            far_out[:, cols] = lax.dot_general(
                spread, far_q[:, cols], (((0,), (0,)), ((), ())), preferred_element_type=F32
            ).astype(BF16)
        far_out_copy().start()

    def shared_copies():
        copies = []
        for k in range(1, XN):
            for crel, (cols, core) in enumerate(((half, r), (other, 1 - r))):
                copies.append(
                    remote(
                        sh_buf.at[pl.ds(TOK // 2 * k, TOK // 2), pl.ds(cols, HALF)],
                        s_in.at[k, pl.ds(here_rows, TOK // 2), :],
                        ssend_sem.at[k, crel], srecv_sem.at[0], at(dx=-k, core=core),
                    )
                )
        copies.append(
            remote(
                sh_buf.at[pl.ds(0, TOK // 2), pl.ds(other, HALF)],
                s_in.at[0, pl.ds(here_rows, TOK // 2), :],
                ssend_sem.at[0, 0], srecv_sem.at[1], partner,
            )
        )
        return copies

    def shared():
        for k in range(1, XN):
            x_copy(k).wait_recv()

        both = jnp.dot(t_buf[...], sgu[...], preferred_element_type=F32)
        sh_hidden[...] = (jax.nn.silu(both[:, : 2 * SF]) * both[:, 2 * SF :]).astype(BF16)
        sh_buf[...] = jnp.dot(sh_hidden[...], sd[...], preferred_element_type=F32).astype(BF16)
        for copy in shared_copies():
            copy.start()
        s_in[0, pl.ds(here_rows, TOK // 2), :] = sh_buf[pl.ds(0, TOK // 2), pl.ds(half, HALF)]

    def combined(d):
        await_bytes(q_buf.at[d, pl.ds(CAP, CAP * len(back_along_y(d))), :], brecv_sem.at[d])

        @pl.when(r != owner(d))
        def _():
            await_bytes(q_buf.at[d, pl.ds(0, CAP), :], brecv0_sem.at[d])

        spread = spreads(lambda expert: code[d, pl.ds(expert, 1), :], [expert_at(dy=k) for k in (0,) + back_along_y(d)])
        rows = pl.ds(0, CAP * (1 + len(back_along_y(d))))
        return [
            lax.dot_general(
                spread, q_buf[d, rows, pl.ds(part * QUARTER, QUARTER)], (((0,), (0,)), ((), ())),
                preferred_element_type=F32,
            )
            for part in range(2)
        ]

    def r_copy(step, way, part):
        outgoing, incoming = (plus_out, plus_in) if way == 0 else (minus_out, minus_in)
        cols = pl.ds(part * QUARTER, QUARTER)
        return remote(
            outgoing.at[step, :, cols], incoming.at[step, :, cols],
            rsend_sem.at[way, part, step], rrecv_sem.at[way, part, step], at(dz=1 if way == 0 else -1),
        )

    def loaded(first, last):
        for i in range(first, last):
            pltpu.make_async_copy(loads[i][0], loads[i][1], load_sem.at[i]).wait()
            weight_copy(i).wait_recv()

    dispatch(0)
    for copy in far_copies():
        copy.start()
    z_arrived(1)
    dispatch(1)
    dispatch(7)
    far_pick()
    weight_copy(0).start()
    for k in range(1, XN):
        x_copy(k).start()
    z_arrived(2)
    dispatch(2)
    dispatch(6)
    weight_copy(1).start()
    weight_copy(2).start()
    z_arrived(3)
    dispatch(3)
    dispatch(5)
    far_pick_two()
    loaded(0, 3)
    experts(0)
    give_far(0)
    z_arrived(4)
    dispatch(4)
    for i in range(3, 6):
        weight_copy(i).start()
    experts(1)
    give_far(1)
    experts(2)
    give_far(2)
    give_back(2, (1,))
    experts(3)
    give_far(3)
    give_back(3)
    loaded(3, 6)
    shared()

    sums = combined(4)
    for way in range(2):
        outgoing = plus_out if way == 0 else minus_out
        outgoing[0, :, pl.ds(way * QUARTER, QUARTER)] = sums[way].astype(BF16)
        r_copy(0, way, way).start()
    give_back(2, (0,))
    give_back(1, (1,))
    for step in range(1, 4):
        both = [combined(4 - step), combined(4 + step)]
        for i in range(2):
            for way in range(2):
                part = 1 - i if way == 0 else i
                outgoing, incoming = (plus_out, plus_in) if way == 0 else (minus_out, minus_in)
                cols = pl.ds(part * QUARTER, QUARTER)
                total = both[way][part]
                if step > 1 or part == way:
                    r_copy(step - 1, way, part).wait_recv()
                    total = total + incoming[step - 1, :, cols].astype(F32)
                outgoing[step, :, cols] = total.astype(BF16)
                r_copy(step, way, part).start()
        if step == 1:
            give_back(1, (0,))
            give_back(0)
            far_sum()

    sums = combined(0)
    await_bytes(s_in.at[pl.ds(1, XN - 1)], srecv_sem.at[0])
    await_bytes(s_in.at[0, pl.ds(other_rows, TOK // 2), :], srecv_sem.at[1])
    far_out_copy().wait_recv()
    for part in range(2):
        cols = pl.ds(part * QUARTER, QUARTER)
        total = far_in[:, cols].astype(F32)
        for i in range(XN):
            total = total + s_in[i, :, cols].astype(F32)
        both[part] = total + sums[part]
    for way, part in ((0, 1), (1, 0), (0, 0), (1, 1)):
        r_copy(3, way, part).wait_recv()
        incoming = plus_in if way == 0 else minus_in
        both[part] = both[part] + incoming[3, :, pl.ds(part * QUARTER, QUARTER)].astype(F32)
    for part in range(2):
        out[:, pl.ds(part * QUARTER, QUARTER)] = both[part].astype(BF16)

    for i in range(6):
        weight_copy(i).wait_send()
    for k in range(1, XN):
        x_copy(k).wait_send()
    for k in range(1, ZN // 2 + 1):
        for piece in z_pieces(k):
            for copy in z_copies(k, *piece):
                copy.wait_send()
    for step in range(4):
        for piece in z_pieces(4 - step):
            r_copy(step, *piece).wait_send()
    for d in range(ZN):
        await_bytes(d_buf.at[d, pl.ds(CAP, CAP * len(along_y(d))), :], ysend_sem.at[d])

        @pl.when(r != owner(d))
        def _():
            y_own_copy(d).wait_send()

    for j in range(ZN // 2):
        for core, d in ((0, j), (1, ZN - 1 - j)):

            @pl.when(r == core)
            def _():
                await_bytes(o_buf.at[pl.ds(ROWS * j + CAP, CAP * len(back_along_y(d))), :], bsend_sem.at[j])
                back_own_copy(j, d).wait_send()
                if d in FAR:
                    for copy in far_back_copies(j, d):
                        copy.wait_send()

    for copy in far_copies() + [far_out_copy()]:
        copy.wait_send()
    for i in range(1, len(NEAR)):
        far_row_copy(i).wait_send()

    @pl.when(r == 1)
    def _():
        far_row_copy(0).wait_send()

    for copy in shared_copies():
        copy.wait_send()


def on_device(*args):
    tokens, norm_gain, expert_ids, route_weights, *rest = args
    vmem = pl.BlockSpec(memory_space=pltpu.VMEM)
    hbm = pl.BlockSpec(memory_space=pl.ANY)
    dma = lambda *shape: pltpu.SemaphoreType.DMA(shape)
    half_z = ZN // 2
    return pl.pallas_call(
        kernel,
        out_shape=jax.ShapeDtypeStruct((TOK, HALF), BF16),
        in_specs=[vmem] * 4 + [hbm] * 6,
        out_specs=vmem,
        scratch_shapes=[
            pltpu.VMEM((XN * TOK // 2, D), BF16),
            pltpu.VMEM((ZN, TOK, HALF), BF16),
            pltpu.VMEM((ZN, EXPERTS, TOK), F32),
            pltpu.VMEM((ZN, ROWS, HALF), BF16),
            pltpu.VMEM((half_z * ROWS, D), BF16),
            pltpu.VMEM((ROWS, FF), BF16),
            pltpu.VMEM((half_z * ROWS, D), BF16),
            pltpu.VMEM((ZN, ROWS, HALF), BF16),
            pltpu.VMEM((TOK, HALF), BF16),
            pltpu.VMEM((EXPERTS, TOK), F32),
            pltpu.VMEM((CAP * len(NEAR), HALF), BF16),
            pltpu.VMEM((CAP * len(FAR), HALF), BF16),
            pltpu.VMEM((TOK, HALF), BF16),
            pltpu.VMEM((TOK, HALF), BF16),
            pltpu.VMEM((4, TOK, HALF), BF16),
            pltpu.VMEM((4, TOK, HALF), BF16),
            pltpu.VMEM((4, TOK, HALF), BF16),
            pltpu.VMEM((4, TOK, HALF), BF16),
            pltpu.VMEM((XN * TOK // 2, 2 * SF), BF16),
            pltpu.VMEM((XN * TOK // 2, D), BF16),
            pltpu.VMEM((XN, TOK, HALF), BF16),
            pltpu.VMEM((D, 2 * FF), BF16),
            pltpu.VMEM((FF, D), BF16),
            pltpu.VMEM((D, 4 * SF), BF16),
            pltpu.VMEM((2 * SF, D), BF16),
            dma(6), dma(6), dma(6),
            dma(2, 2, 4), dma(2, 2, 4), dma(2, 4), dma(2, 4),
            dma(ZN), dma(half_z), dma(ZN), dma(half_z),
            dma(half_z), dma(ZN), dma(half_z), dma(ZN),
            dma(2, 2, 4), dma(2, 2, 4),
            dma(3), dma(3), dma(XN, 2), dma(2),
            dma(3), dma(3), dma(5), dma(half_z), dma(half_z, 2), dma(len(FAR)),
        ],
        compiler_params=pltpu.CompilerParams(
            collective_id=0, has_side_effects=True, vmem_limit_bytes=63 * 2**20
        ),
    )(tokens, norm_gain, expert_ids.T, route_weights.T, *rest)


def solution(mesh):
    placed = (
        P(("dp", "expert"), None),
        P(),
        P(("dp", "expert"), None),
        P(("dp", "expert"), None),
        P("expert", None, "tensor"),
        P("expert", None, "tensor"),
        P("expert", "tensor", None),
        P(None, ("dp", "tensor")),
        P(None, ("dp", "tensor")),
        P(("dp", "tensor"), None),
    )
    return jax.shard_map(
        on_device,
        mesh=mesh,
        in_specs=placed,
        out_specs=P(("dp", "expert"), "tensor"),
        check_vma=False,
    )
```

```python
import jax
import jax.numpy as jnp
from jax import lax
from jax.experimental import pallas as pl
from jax.experimental.pallas import tpu as pltpu
from jax.sharding import PartitionSpec as P

D = 2560
HALF = D // 2
QUARTER = HALF // 2
FF2 = 384
FF = 768
SF = 256
EXPERTS = 32
TOP = 6
TOK = 128
CAP = 48
YN = 4
ZN = 8
XN = 4
ROWS = YN * CAP
EPSILON = 1e-06
MESH = pl.DeviceIdType.MESH
ORDER = (0, 1, 3, 2)
PLACE = {k: CAP * ORDER.index(k) for k in ORDER}
FAR = (0, 7, 1, 6, 2, 5, 3)
NEAR = (0, 7, 1, 6, 2)
BF16 = jnp.bfloat16
F32 = jnp.float32


def owner(d):
    return 0 if d < ZN // 2 else 1


def signed(d):
    return d if d <= ZN // 2 else d - ZN


def along_y(d):
    return (1, 3) if d in NEAR else (1, 3, 2)


def back_along_y(d):
    return (1, 3) if d in FAR else (1, 3, 2)


def chunk_of(d):
    return d if d < ZN // 2 else ZN - 1 - d


def kernel(
    tokens, gain, ids, weights, wg_in, wu_in, wd_in, sg_in, su_in, sd_in,
    out,
    t_buf, g_buf, code, d_buf, r_buf, h_buf, o_buf, q_buf,
    far_tok, far_code, far_rows, far_q, far_out, far_in,
    plus_in, minus_in, plus_out, minus_out, sh_hidden, sh_buf, s_in,
    wgu, wd, sgu, sd,
    load_sem, wsend_sem, wrecv_sem,
    zsend_sem, zrecv_sem, csend_sem, crecv_sem,
    ysend_sem, yrecv_sem, ysend0_sem, yrecv0_sem,
    bsend_sem, brecv_sem, bsend0_sem, brecv0_sem,
    rsend_sem, rrecv_sem,
    xsend_sem, xrecv_sem, ssend_sem, srecv_sem,
    fsend_sem, frecv_sem, fdsend_sem, fdrecv_sem, fbsend_sem, fbrecv_sem,
):
    x = lax.axis_index("dp")
    e = lax.axis_index("expert")
    r = lax.axis_index("tensor")
    y = e // ZN
    z = e % ZN
    half = pl.multiple_of(r * HALF, 128)
    other = pl.multiple_of((1 - r) * HALF, 128)

    def at(dx=0, dy=0, dz=0, core=None):
        return (
            (x + dx + XN) % XN,
            ((y + dy + YN) % YN) * ZN + (z + dz + ZN) % ZN,
            r if core is None else core,
        )

    partner = at(core=1 - r)
    here_rows = pl.multiple_of(r * (TOK // 2), TOK // 2)
    other_rows = pl.multiple_of((1 - r) * (TOK // 2), TOK // 2)

    def remote(src, dst, send, recv, device):
        return pltpu.make_async_remote_copy(
            src_ref=src, dst_ref=dst, send_sem=send, recv_sem=recv,
            device_id=device, device_id_type=MESH,
        )

    def await_bytes(ref, sem):
        pltpu.make_async_copy(ref, ref, sem).wait()

    barrier = pltpu.get_barrier_semaphore()
    peers = [partner]
    for k in sorted({signed(d) for d in FAR} - {0}):
        peers += [at(dz=k), at(dz=k, core=1 - r)]
    for k in range(1, YN):
        peers += [at(dy=k), at(dy=k, core=1 - r)]
    for k in range(1, XN):
        peers += [at(dx=k), at(dx=k, core=1 - r)]
    for peer in peers:
        pl.semaphore_signal(barrier, inc=1, device_id=peer, device_id_type=MESH)

    loads = [
        (wg_in.at[0], wgu.at[:, pl.ds(0, FF2)]),
        (wu_in.at[0], wgu.at[:, pl.ds(FF, FF2)]),
        (wd_in.at[0], wd.at[pl.ds(0, FF2), :]),
        (sg_in, sgu.at[:, pl.ds(0, SF)]),
        (su_in, sgu.at[:, pl.ds(2 * SF, SF)]),
        (sd_in, sd.at[pl.ds(0, SF), :]),
    ]
    for i, (src, dst) in enumerate(loads):
        pltpu.make_async_copy(src, dst, load_sem.at[i]).start()

    gain_row = gain[...].reshape(1, D)

    def norm_step(i, carry):
        rows = pl.ds(pl.multiple_of(i * 16, 16), 16)
        values = tokens[rows, :].astype(F32)
        inverse = lax.rsqrt(jnp.mean(values * values, axis=1, keepdims=True) + EPSILON)
        normed = values * inverse * gain_row
        @pl.when(i // 4 == r)
        def _():
            t_buf[pl.ds(pl.multiple_of((i % 4) * 16, 16), 16), :] = normed.astype(BF16)

        g_buf[0, rows, :] = jnp.where(r == 0, normed[:, :HALF], normed[:, HALF:]).astype(BF16)
        return carry

    lax.fori_loop(0, TOK // 16, norm_step, 0)

    expert_row = lax.broadcasted_iota(jnp.int32, (EXPERTS, TOK), 0)
    named = jnp.zeros((EXPERTS, TOK), F32)
    weight = jnp.zeros((EXPERTS, TOK), F32)
    for k in range(TOP):
        match = ids[k : k + 1, :] == expert_row
        named = jnp.where(match, 1.0, named)
        weight = jnp.where(match, weights[k : k + 1, :].astype(F32), weight)
    before = lax.broadcasted_iota(jnp.int32, (TOK, TOK), 0) < lax.broadcasted_iota(jnp.int32, (TOK, TOK), 1)
    earlier = jnp.where(before, 1.0, 0.0).astype(BF16)
    rank = jnp.dot(named.astype(BF16), earlier, preferred_element_type=F32)
    code[0] = jnp.where(named > 0.5, weight * 64.0 + rank, -1.0)

    pl.semaphore_wait(barrier, len(peers))

    def z_pieces(k):
        return [(way, part) for part in range(2) for way in range(2) if k < ZN // 2 or way == part]

    def z_copies(k, way, part):
        if way == 0:
            here, there, to = k - 1, k, at(dz=-1)
        else:
            here, there, to = (ZN - (k - 1)) % ZN, ZN - k, at(dz=1)
        cols = pl.ds(part * QUARTER, QUARTER)
        copies = [
            remote(
                g_buf.at[here, :, cols], g_buf.at[there, :, cols],
                zsend_sem.at[way, part, k - 1], zrecv_sem.at[way, part, k - 1], to,
            )
        ]
        if part == 0 and (k < ZN // 2 or way == 0):
            copies.append(
                remote(code.at[here], code.at[there], csend_sem.at[way, k - 1], crecv_sem.at[way, k - 1], to)
            )
        return copies

    partner_places = [
        wgu.at[:, pl.ds(FF2, FF2)],
        wgu.at[:, pl.ds(FF + FF2, FF2)],
        wd.at[pl.ds(FF2, FF2), :],
        sgu.at[:, pl.ds(SF, SF)],
        sgu.at[:, pl.ds(3 * SF, SF)],
        sd.at[pl.ds(SF, SF), :],
    ]

    def weight_copy(i):
        return remote(loads[i][0], partner_places[i], wsend_sem.at[i], wrecv_sem.at[i], partner)

    def x_copy(k):
        return remote(t_buf.at[pl.ds(0, TOK // 2)], t_buf.at[pl.ds(TOK // 2 * k, TOK // 2)], xsend_sem.at[k - 1], xrecv_sem.at[k - 1], at(dx=k))

    for piece in z_pieces(1):
        for copy in z_copies(1, *piece):
            copy.start()

    slot = lax.broadcasted_iota(jnp.int32, (CAP, TOK), 0).astype(F32)

    def slot_parts(line_of, experts):
        for expert in experts:
            line = line_of(expert)
            scale = jnp.floor(line * (1.0 / 64.0))
            yield slot == line - 64.0 * scale, scale * (1.0 / 64.0)

    def picks(line_of, experts):
        return jnp.concatenate(
            [jnp.where(hit, 1.0, 0.0) for hit, _ in slot_parts(line_of, experts)], axis=0
        ).astype(BF16)

    def spreads(line_of, experts):
        return jnp.concatenate(
            [jnp.where(hit, scale, 0.0) for hit, scale in slot_parts(line_of, experts)], axis=0
        ).astype(BF16)

    def expert_at(dy=0, dz=0):
        return ((y + dy + YN) % YN) * ZN + (z + dz + ZN) % ZN

    def y_experts(d):
        return [expert_at(dy=k) for k in ORDER if k == 0 or k in along_y(d)]

    def y_copies(d):
        j, core = chunk_of(d), owner(d)
        return [
            remote(
                d_buf.at[d, pl.ds(PLACE[k], CAP), :],
                r_buf.at[pl.ds(ROWS * j + PLACE[k], CAP), pl.ds(half, HALF)],
                ysend_sem.at[d], yrecv_sem.at[j], at(dy=k, core=core),
            )
            for k in along_y(d)
        ]

    def y_own_copy(d):
        return remote(
            d_buf.at[d, pl.ds(0, CAP), :],
            r_buf.at[pl.ds(ROWS * chunk_of(d), CAP), pl.ds(half, HALF)],
            ysend0_sem.at[d], yrecv0_sem.at[chunk_of(d)], partner,
        )

    def dispatch(d):
        pick = picks(lambda expert: code[d, pl.ds(expert, 1), :], y_experts(d))
        rows = pl.ds(0, CAP * (1 + len(along_y(d))))
        for cols in (pl.ds(0, QUARTER), pl.ds(QUARTER, QUARTER)):
            d_buf[d, rows, cols] = jnp.dot(pick, g_buf[d, :, cols], preferred_element_type=F32).astype(BF16)
        for copy in y_copies(d):
            copy.start()

        @pl.when(r == owner(d))
        def _():
            r_buf[pl.ds(ROWS * chunk_of(d), CAP), pl.ds(half, HALF)] = d_buf[d, pl.ds(0, CAP), :]

        @pl.when(r != owner(d))
        def _():
            y_own_copy(d).start()

    def far_copies():
        return [
            remote(g_buf.at[0], far_tok, fsend_sem.at[0], frecv_sem.at[0], at(dy=2)),
            remote(code.at[0], far_code, fsend_sem.at[1], frecv_sem.at[1], at(dy=2)),
        ]

    def far_experts(distances):
        return [expert_at(dz=-signed(d)) for d in distances]

    def far_line(expert):
        return far_code[pl.ds(expert, 1), :]

    def far_row_copy(i):
        d = NEAR[i]
        j = chunk_of(d)
        return remote(
            far_rows.at[pl.ds(CAP * i, CAP), :],
            r_buf.at[pl.ds(ROWS * j + PLACE[2], CAP), pl.ds(half, HALF)],
            fdsend_sem.at[i], fdrecv_sem.at[j],
            partner if d == 0 else at(dz=-signed(d), core=owner(d)),
        )

    def far_pick():
        for copy in far_copies():
            copy.wait_recv()
        pick = picks(far_line, far_experts(NEAR))
        for cols in (pl.ds(0, QUARTER), pl.ds(QUARTER, QUARTER)):
            far_rows[:, cols] = jnp.dot(pick, far_tok[:, cols], preferred_element_type=F32).astype(BF16)

        @pl.when(r == 0)
        def _():
            r_buf[pl.ds(PLACE[2], CAP), pl.ds(half, HALF)] = far_rows[pl.ds(0, CAP), :]

        @pl.when(r == 1)
        def _():
            far_row_copy(0).start()

        for i in (1, 2):
            far_row_copy(i).start()

    def far_pick_two():
        for i in range(3, len(NEAR)):
            far_row_copy(i).start()

    def z_arrived(k):
        for piece in z_pieces(k):
            for copy in z_copies(k, *piece):
                copy.wait_recv()
            if k < ZN // 2 and piece in z_pieces(k + 1):
                for copy in z_copies(k + 1, *piece):
                    copy.start()

    def experts(*chunks):
        for core, j in enumerate(chunks):
            d = j if core == 0 else ZN - 1 - j

            @pl.when(r == core)
            def _():
                await_bytes(r_buf.at[pl.ds(ROWS * j, CAP), pl.ds(other, HALF)], yrecv0_sem.at[j])
                await_bytes(r_buf.at[pl.ds(ROWS * j + CAP, CAP * len(along_y(d))), :], yrecv_sem.at[j])
                if d == 0:
                    await_bytes(r_buf.at[pl.ds(ROWS * j + PLACE[2], CAP), pl.ds(other, HALF)], fdrecv_sem.at[j])
                elif d in NEAR:
                    await_bytes(r_buf.at[pl.ds(ROWS * j + PLACE[2], CAP), :], fdrecv_sem.at[j])

        rows = pl.ds(pl.multiple_of(ROWS * jnp.where(r == 0, chunks[0], chunks[1]), 16), ROWS)
        both = jnp.dot(r_buf[rows, :], wgu[...], preferred_element_type=F32)
        h_buf[...] = (jax.nn.silu(both[:, :FF]) * both[:, FF:]).astype(BF16)
        o_buf[rows, :] = jnp.dot(h_buf[...], wd[...], preferred_element_type=F32).astype(BF16)

    def back_copies(j, d):
        copies = []
        for k in back_along_y(d):
            for cols, core in ((half, r), (other, 1 - r)):
                copies.append(
                    remote(
                        o_buf.at[pl.ds(ROWS * j + PLACE[k], CAP), pl.ds(cols, HALF)],
                        q_buf.at[d, pl.ds(PLACE[k], CAP), :],
                        bsend_sem.at[j], brecv_sem.at[d], at(dy=-k, core=core),
                    )
                )
        return copies

    def back_own_copy(j, d):
        return remote(
            o_buf.at[pl.ds(ROWS * j, CAP), pl.ds(other, HALF)], q_buf.at[d, pl.ds(0, CAP), :],
            bsend0_sem.at[j], brecv0_sem.at[d], partner,
        )

    def far_back_copies(j, d):
        i = FAR.index(d)
        copies = []
        for cols, core in ((half, r), (other, 1 - r)):
            if d == 0 and core is r:
                continue
            copies.append(
                remote(
                    o_buf.at[pl.ds(ROWS * j + PLACE[2], CAP), pl.ds(cols, HALF)],
                    far_q.at[pl.ds(CAP * i, CAP), :],
                    fbsend_sem.at[j, 0 if core is r else 1], fbrecv_sem.at[i], at(dz=signed(d), core=core),
                )
            )
        return copies

    def give_back(*chunks):
        for core, j in enumerate(chunks):
            if j is None:
                continue
            d = j if core == 0 else ZN - 1 - j

            @pl.when(r == core)
            def _():
                for copy in back_copies(j, d):
                    copy.start()
                back_own_copy(j, d).start()
                q_buf[d, pl.ds(0, CAP), :] = o_buf[pl.ds(ROWS * j, CAP), pl.ds(half, HALF)]

    def give_far(*chunks):
        for core, j in enumerate(chunks):
            d = j if core == 0 else ZN - 1 - j

            @pl.when(r == core)
            def _():
                if d in FAR:
                    for copy in far_back_copies(j, d):
                        copy.start()
                if d == 0:
                    far_q[pl.ds(0, CAP), :] = o_buf[pl.ds(PLACE[2], CAP), pl.ds(half, HALF)]

    def far_out_copy():
        return remote(far_out, far_in, fsend_sem.at[2], frecv_sem.at[2], at(dy=2))

    def far_sum():
        @pl.when(r == 1)
        def _():
            await_bytes(far_q.at[pl.ds(0, CAP), :], fbrecv_sem.at[0])

        for i in range(1, len(FAR)):
            await_bytes(far_q.at[pl.ds(CAP * i, CAP), :], fbrecv_sem.at[i])
        spread = spreads(far_line, far_experts(FAR))
        for cols in (pl.ds(0, QUARTER), pl.ds(QUARTER, QUARTER)):
            far_out[:, cols] = lax.dot_general(
                spread, far_q[:, cols], (((0,), (0,)), ((), ())), preferred_element_type=F32
            ).astype(BF16)
        far_out_copy().start()

    def shared_copies():
        copies = []
        for k in range(1, XN):
            for crel, (cols, core) in enumerate(((half, r), (other, 1 - r))):
                copies.append(
                    remote(
                        sh_buf.at[pl.ds(TOK // 2 * k, TOK // 2), pl.ds(cols, HALF)],
                        s_in.at[k, pl.ds(here_rows, TOK // 2), :],
                        ssend_sem.at[k, crel], srecv_sem.at[0], at(dx=-k, core=core),
                    )
                )
        copies.append(
            remote(
                sh_buf.at[pl.ds(0, TOK // 2), pl.ds(other, HALF)],
                s_in.at[0, pl.ds(here_rows, TOK // 2), :],
                ssend_sem.at[0, 0], srecv_sem.at[1], partner,
            )
        )
        return copies

    def shared():
        for k in range(1, XN):
            x_copy(k).wait_recv()

        both = jnp.dot(t_buf[...], sgu[...], preferred_element_type=F32)
        sh_hidden[...] = (jax.nn.silu(both[:, : 2 * SF]) * both[:, 2 * SF :]).astype(BF16)
        sh_buf[...] = jnp.dot(sh_hidden[...], sd[...], preferred_element_type=F32).astype(BF16)
        for copy in shared_copies():
            copy.start()
        s_in[0, pl.ds(here_rows, TOK // 2), :] = sh_buf[pl.ds(0, TOK // 2), pl.ds(half, HALF)]

    def combined(d):
        await_bytes(q_buf.at[d, pl.ds(CAP, CAP * len(back_along_y(d))), :], brecv_sem.at[d])

        @pl.when(r != owner(d))
        def _():
            await_bytes(q_buf.at[d, pl.ds(0, CAP), :], brecv0_sem.at[d])

        spread = spreads(lambda expert: code[d, pl.ds(expert, 1), :], [expert_at(dy=k) for k in (0,) + back_along_y(d)])
        rows = pl.ds(0, CAP * (1 + len(back_along_y(d))))
        return [
            lax.dot_general(
                spread, q_buf[d, rows, pl.ds(part * QUARTER, QUARTER)], (((0,), (0,)), ((), ())),
                preferred_element_type=F32,
            )
            for part in range(2)
        ]

    def r_copy(step, way, part):
        outgoing, incoming = (plus_out, plus_in) if way == 0 else (minus_out, minus_in)
        cols = pl.ds(part * QUARTER, QUARTER)
        return remote(
            outgoing.at[step, :, cols], incoming.at[step, :, cols],
            rsend_sem.at[way, part, step], rrecv_sem.at[way, part, step], at(dz=1 if way == 0 else -1),
        )

    def loaded(first, last):
        for i in range(first, last):
            pltpu.make_async_copy(loads[i][0], loads[i][1], load_sem.at[i]).wait()
            weight_copy(i).wait_recv()

    dispatch(0)
    for copy in far_copies():
        copy.start()
    z_arrived(1)
    dispatch(1)
    dispatch(7)
    weight_copy(0).start()
    for k in range(1, XN):
        x_copy(k).start()
    z_arrived(2)
    dispatch(2)
    dispatch(6)
    weight_copy(1).start()
    weight_copy(2).start()
    z_arrived(3)
    dispatch(5)
    dispatch(3)
    loaded(0, 3)
    z_arrived(4)
    dispatch(4)
    far_pick()
    far_pick_two()
    for i in range(3, 6):
        weight_copy(i).start()
    experts(0, 0)
    give_far(0, 0)
    experts(1, 2)
    give_far(1, 2)
    give_back(None, 2)
    experts(3, 3)
    give_far(3, 3)
    give_back(3, 3)
    experts(2, 1)
    give_far(2, 1)
    give_back(2, 1)
    loaded(3, 6)
    shared()

    sums = combined(4)
    for way in range(2):
        outgoing = plus_out if way == 0 else minus_out
        outgoing[0, :, pl.ds(way * QUARTER, QUARTER)] = sums[way].astype(BF16)
        r_copy(0, way, way).start()
    for step in range(1, 4):
        both = [combined(4 - step), combined(4 + step)]
        for i in range(2):
            for way in range(2):
                part = 1 - i if way == 0 else i
                outgoing, incoming = (plus_out, plus_in) if way == 0 else (minus_out, minus_in)
                cols = pl.ds(part * QUARTER, QUARTER)
                total = both[way][part]
                if step > 1 or part == way:
                    r_copy(step - 1, way, part).wait_recv()
                    total = total + incoming[step - 1, :, cols].astype(F32)
                outgoing[step, :, cols] = total.astype(BF16)
                r_copy(step, way, part).start()
        if step == 1:
            give_back(1, 0)
            give_back(0, None)
            far_sum()

    sums = combined(0)
    await_bytes(s_in.at[pl.ds(1, XN - 1)], srecv_sem.at[0])
    await_bytes(s_in.at[0, pl.ds(other_rows, TOK // 2), :], srecv_sem.at[1])
    far_out_copy().wait_recv()
    for part in range(2):
        cols = pl.ds(part * QUARTER, QUARTER)
        total = far_in[:, cols].astype(F32)
        for i in range(XN):
            total = total + s_in[i, :, cols].astype(F32)
        both[part] = total + sums[part]
    for way, part in ((0, 1), (1, 0), (0, 0), (1, 1)):
        r_copy(3, way, part).wait_recv()
        incoming = plus_in if way == 0 else minus_in
        both[part] = both[part] + incoming[3, :, pl.ds(part * QUARTER, QUARTER)].astype(F32)
    for part in range(2):
        out[:, pl.ds(part * QUARTER, QUARTER)] = both[part].astype(BF16)

    for i in range(6):
        weight_copy(i).wait_send()
    for k in range(1, XN):
        x_copy(k).wait_send()
    for k in range(1, ZN // 2 + 1):
        for piece in z_pieces(k):
            for copy in z_copies(k, *piece):
                copy.wait_send()
    for step in range(4):
        for piece in z_pieces(4 - step):
            r_copy(step, *piece).wait_send()
    for d in range(ZN):
        await_bytes(d_buf.at[d, pl.ds(CAP, CAP * len(along_y(d))), :], ysend_sem.at[d])

        @pl.when(r != owner(d))
        def _():
            y_own_copy(d).wait_send()

    for j in range(ZN // 2):
        for core, d in ((0, j), (1, ZN - 1 - j)):

            @pl.when(r == core)
            def _():
                await_bytes(o_buf.at[pl.ds(ROWS * j + CAP, CAP * len(back_along_y(d))), :], bsend_sem.at[j])
                back_own_copy(j, d).wait_send()
                if d in FAR:
                    for copy in far_back_copies(j, d):
                        copy.wait_send()

    for copy in far_copies() + [far_out_copy()]:
        copy.wait_send()
    for i in range(1, len(NEAR)):
        far_row_copy(i).wait_send()

    @pl.when(r == 1)
    def _():
        far_row_copy(0).wait_send()

    for copy in shared_copies():
        copy.wait_send()


def on_device(*args):
    tokens, norm_gain, expert_ids, route_weights, *rest = args
    vmem = pl.BlockSpec(memory_space=pltpu.VMEM)
    hbm = pl.BlockSpec(memory_space=pl.ANY)
    dma = lambda *shape: pltpu.SemaphoreType.DMA(shape)
    half_z = ZN // 2
    return pl.pallas_call(
        kernel,
        out_shape=jax.ShapeDtypeStruct((TOK, HALF), BF16),
        in_specs=[vmem] * 4 + [hbm] * 6,
        out_specs=vmem,
        scratch_shapes=[
            pltpu.VMEM((XN * TOK // 2, D), BF16),
            pltpu.VMEM((ZN, TOK, HALF), BF16),
            pltpu.VMEM((ZN, EXPERTS, TOK), F32),
            pltpu.VMEM((ZN, ROWS, HALF), BF16),
            pltpu.VMEM((half_z * ROWS, D), BF16),
            pltpu.VMEM((ROWS, FF), BF16),
            pltpu.VMEM((half_z * ROWS, D), BF16),
            pltpu.VMEM((ZN, ROWS, HALF), BF16),
            pltpu.VMEM((TOK, HALF), BF16),
            pltpu.VMEM((EXPERTS, TOK), F32),
            pltpu.VMEM((CAP * len(NEAR), HALF), BF16),
            pltpu.VMEM((CAP * len(FAR), HALF), BF16),
            pltpu.VMEM((TOK, HALF), BF16),
            pltpu.VMEM((TOK, HALF), BF16),
            pltpu.VMEM((4, TOK, HALF), BF16),
            pltpu.VMEM((4, TOK, HALF), BF16),
            pltpu.VMEM((4, TOK, HALF), BF16),
            pltpu.VMEM((4, TOK, HALF), BF16),
            pltpu.VMEM((XN * TOK // 2, 2 * SF), BF16),
            pltpu.VMEM((XN * TOK // 2, D), BF16),
            pltpu.VMEM((XN, TOK, HALF), BF16),
            pltpu.VMEM((D, 2 * FF), BF16),
            pltpu.VMEM((FF, D), BF16),
            pltpu.VMEM((D, 4 * SF), BF16),
            pltpu.VMEM((2 * SF, D), BF16),
            dma(6), dma(6), dma(6),
            dma(2, 2, 4), dma(2, 2, 4), dma(2, 4), dma(2, 4),
            dma(ZN), dma(half_z), dma(ZN), dma(half_z),
            dma(half_z), dma(ZN), dma(half_z), dma(ZN),
            dma(2, 2, 4), dma(2, 2, 4),
            dma(3), dma(3), dma(XN, 2), dma(2),
            dma(3), dma(3), dma(len(NEAR)), dma(half_z), dma(half_z, 2), dma(len(FAR)),
        ],
        compiler_params=pltpu.CompilerParams(
            collective_id=0, has_side_effects=True, vmem_limit_bytes=63 * 2**20
        ),
    )(tokens, norm_gain, expert_ids.T, route_weights.T, *rest)


def solution(mesh):
    placed = (
        P(("dp", "expert"), None),
        P(),
        P(("dp", "expert"), None),
        P(("dp", "expert"), None),
        P("expert", None, "tensor"),
        P("expert", None, "tensor"),
        P("expert", "tensor", None),
        P(None, ("dp", "tensor")),
        P(None, ("dp", "tensor")),
        P(("dp", "tensor"), None),
    )
    return jax.shard_map(
        on_device,
        mesh=mesh,
        in_specs=placed,
        out_specs=P(("dp", "expert"), "tensor"),
        check_vma=False,
    )
```

```python
import jax
import jax.numpy as jnp
from jax import lax
from jax.experimental import pallas as pl
from jax.experimental.pallas import tpu as pltpu
from jax.sharding import PartitionSpec as P

D = 2560
HALF = D // 2
QUARTER = HALF // 2
FF2 = 384
FF = 768
SF = 256
EXPERTS = 32
TOP = 6
TOK = 128
CAP = 48
YN = 4
ZN = 8
XN = 4
ROWS = YN * CAP
EPSILON = 1e-06
MESH = pl.DeviceIdType.MESH
ORDER = (0, 1, 3, 2)
PLACE = {k: CAP * ORDER.index(k) for k in ORDER}
FAR = (0, 7, 1, 6, 2, 5, 3)
NEAR = (0, 7, 1, 6, 2)
BF16 = jnp.bfloat16
F32 = jnp.float32


def owner(d):
    return 0 if d < ZN // 2 else 1


def signed(d):
    return d if d <= ZN // 2 else d - ZN


def along_y(d):
    return (1, 3) if d in NEAR else (1, 3, 2)


def back_along_y(d):
    return (1, 3) if d in FAR else (1, 3, 2)


def chunk_of(d):
    return d if d < ZN // 2 else ZN - 1 - d


def kernel(
    tokens, gain, ids, weights, wg_in, wu_in, wd_in, sg_in, su_in, sd_in,
    out,
    t_buf, g_buf, code, d_buf, r_buf, h_buf, o_buf, q_buf,
    far_tok, far_code, far_rows, far_q, far_out, far_in,
    plus_in, minus_in, plus_out, minus_out, sh_hidden, sh_buf, s_in,
    wgu, wd, sgu, sd,
    load_sem, wsend_sem, wrecv_sem,
    zsend_sem, zrecv_sem, csend_sem, crecv_sem,
    ysend_sem, yrecv_sem, ysend0_sem, yrecv0_sem,
    bsend_sem, brecv_sem, bsend0_sem, brecv0_sem,
    rsend_sem, rrecv_sem,
    xsend_sem, xrecv_sem, ssend_sem, srecv_sem,
    fsend_sem, frecv_sem, fdsend_sem, fdrecv_sem, fbsend_sem, fbrecv_sem,
):
    x = lax.axis_index("dp")
    e = lax.axis_index("expert")
    r = lax.axis_index("tensor")
    y = e // ZN
    z = e % ZN
    half = pl.multiple_of(r * HALF, 128)
    other = pl.multiple_of((1 - r) * HALF, 128)

    def at(dx=0, dy=0, dz=0, core=None):
        return (
            (x + dx + XN) % XN,
            ((y + dy + YN) % YN) * ZN + (z + dz + ZN) % ZN,
            r if core is None else core,
        )

    partner = at(core=1 - r)
    here_rows = pl.multiple_of(r * (TOK // 2), TOK // 2)
    other_rows = pl.multiple_of((1 - r) * (TOK // 2), TOK // 2)

    def remote(src, dst, send, recv, device):
        return pltpu.make_async_remote_copy(
            src_ref=src, dst_ref=dst, send_sem=send, recv_sem=recv,
            device_id=device, device_id_type=MESH,
        )

    def await_bytes(ref, sem):
        pltpu.make_async_copy(ref, ref, sem).wait()

    barrier = pltpu.get_barrier_semaphore()
    peers = [partner]
    for k in sorted({signed(d) for d in FAR} - {0}):
        peers += [at(dz=k), at(dz=k, core=1 - r)]
    for k in range(1, YN):
        peers += [at(dy=k), at(dy=k, core=1 - r)]
    for k in range(1, XN):
        peers += [at(dx=k), at(dx=k, core=1 - r)]
    for peer in peers:
        pl.semaphore_signal(barrier, inc=1, device_id=peer, device_id_type=MESH)

    loads = [
        (wg_in.at[0], wgu.at[:, pl.ds(0, FF2)]),
        (wu_in.at[0], wgu.at[:, pl.ds(FF, FF2)]),
        (wd_in.at[0], wd.at[pl.ds(0, FF2), :]),
        (sg_in, sgu.at[:, pl.ds(0, SF)]),
        (su_in, sgu.at[:, pl.ds(2 * SF, SF)]),
        (sd_in, sd.at[pl.ds(0, SF), :]),
    ]
    for i, (src, dst) in enumerate(loads):
        pltpu.make_async_copy(src, dst, load_sem.at[i]).start()

    gain_row = gain[...].reshape(1, D)

    def norm_step(i, carry):
        rows = pl.ds(pl.multiple_of(i * 16, 16), 16)
        values = tokens[rows, :].astype(F32)
        inverse = lax.rsqrt(jnp.mean(values * values, axis=1, keepdims=True) + EPSILON)
        normed = values * inverse * gain_row
        @pl.when(i // 4 == r)
        def _():
            t_buf[pl.ds(pl.multiple_of((i % 4) * 16, 16), 16), :] = normed.astype(BF16)

        g_buf[0, rows, :] = jnp.where(r == 0, normed[:, :HALF], normed[:, HALF:]).astype(BF16)
        return carry

    lax.fori_loop(0, TOK // 16, norm_step, 0)

    expert_row = lax.broadcasted_iota(jnp.int32, (EXPERTS, TOK), 0)
    named = jnp.zeros((EXPERTS, TOK), F32)
    weight = jnp.zeros((EXPERTS, TOK), F32)
    for k in range(TOP):
        match = ids[k : k + 1, :] == expert_row
        named = jnp.where(match, 1.0, named)
        weight = jnp.where(match, weights[k : k + 1, :].astype(F32), weight)
    before = lax.broadcasted_iota(jnp.int32, (TOK, TOK), 0) < lax.broadcasted_iota(jnp.int32, (TOK, TOK), 1)
    earlier = jnp.where(before, 1.0, 0.0).astype(BF16)
    rank = jnp.dot(named.astype(BF16), earlier, preferred_element_type=F32)
    code[0] = jnp.where(named > 0.5, weight * 64.0 + rank, -1.0)

    pl.semaphore_wait(barrier, len(peers))

    def z_pieces(k):
        return [(way, part) for part in range(2) for way in range(2) if k < ZN // 2 or way == part]

    def z_copies(k, way, part):
        if way == 0:
            here, there, to = k - 1, k, at(dz=-1)
        else:
            here, there, to = (ZN - (k - 1)) % ZN, ZN - k, at(dz=1)
        cols = pl.ds(part * QUARTER, QUARTER)
        copies = [
            remote(
                g_buf.at[here, :, cols], g_buf.at[there, :, cols],
                zsend_sem.at[way, part, k - 1], zrecv_sem.at[way, part, k - 1], to,
            )
        ]
        if part == 0 and (k < ZN // 2 or way == 0):
            copies.append(
                remote(code.at[here], code.at[there], csend_sem.at[way, k - 1], crecv_sem.at[way, k - 1], to)
            )
        return copies

    partner_places = [
        wgu.at[:, pl.ds(FF2, FF2)],
        wgu.at[:, pl.ds(FF + FF2, FF2)],
        wd.at[pl.ds(FF2, FF2), :],
        sgu.at[:, pl.ds(SF, SF)],
        sgu.at[:, pl.ds(3 * SF, SF)],
        sd.at[pl.ds(SF, SF), :],
    ]

    def weight_copy(i):
        return remote(loads[i][0], partner_places[i], wsend_sem.at[i], wrecv_sem.at[i], partner)

    def x_copy(k):
        return remote(t_buf.at[pl.ds(0, TOK // 2)], t_buf.at[pl.ds(TOK // 2 * k, TOK // 2)], xsend_sem.at[k - 1], xrecv_sem.at[k - 1], at(dx=k))

    for piece in z_pieces(1):
        for copy in z_copies(1, *piece):
            copy.start()

    slot = lax.broadcasted_iota(jnp.int32, (CAP, TOK), 0).astype(F32)

    def slot_parts(line_of, experts):
        for expert in experts:
            line = line_of(expert)
            scale = jnp.floor(line * (1.0 / 64.0))
            yield slot == line - 64.0 * scale, scale * (1.0 / 64.0)

    def picks(line_of, experts):
        return jnp.concatenate(
            [jnp.where(hit, 1.0, 0.0) for hit, _ in slot_parts(line_of, experts)], axis=0
        ).astype(BF16)

    def spreads(line_of, experts):
        return jnp.concatenate(
            [jnp.where(hit, scale, 0.0) for hit, scale in slot_parts(line_of, experts)], axis=0
        ).astype(BF16)

    def expert_at(dy=0, dz=0):
        return ((y + dy + YN) % YN) * ZN + (z + dz + ZN) % ZN

    def y_experts(d):
        return [expert_at(dy=k) for k in ORDER if k == 0 or k in along_y(d)]

    def y_copies(d, part):
        j, core = chunk_of(d), owner(d)
        here = pl.ds(part * QUARTER, QUARTER)
        there = pl.ds(pl.multiple_of(half + part * QUARTER, 128), QUARTER)
        return [
            remote(
                d_buf.at[d, pl.ds(PLACE[k], CAP), here],
                r_buf.at[pl.ds(ROWS * j + PLACE[k], CAP), there],
                ysend_sem.at[d], yrecv_sem.at[j], at(dy=k, core=core),
            )
            for k in along_y(d)
        ]

    def dispatch(d, parts=(0, 1)):
        pick = picks(lambda expert: code[d, pl.ds(expert, 1), :], y_experts(d))
        rows = pl.ds(0, CAP * (1 + len(along_y(d))))
        for part in parts:
            here = pl.ds(part * QUARTER, QUARTER)
            there = pl.ds(pl.multiple_of(half + part * QUARTER, 128), QUARTER)
            d_buf[d, rows, here] = jnp.dot(pick, g_buf[d, :, here], preferred_element_type=F32).astype(BF16)
            for copy in y_copies(d, part):
                copy.start()
            own = d_buf.at[d, pl.ds(0, CAP), here]
            own_place = r_buf.at[pl.ds(ROWS * chunk_of(d), CAP), there]

            @pl.when(r == owner(d))
            def _():
                own_place[...] = own[...]

            @pl.when(r != owner(d))
            def _():
                remote(own, own_place, ysend0_sem.at[d], yrecv0_sem.at[chunk_of(d)], partner).start()

    def far_copies():
        return [
            remote(g_buf.at[0], far_tok, fsend_sem.at[0], frecv_sem.at[0], at(dy=2)),
            remote(code.at[0], far_code, fsend_sem.at[1], frecv_sem.at[1], at(dy=2)),
        ]

    def far_experts(distances):
        return [expert_at(dz=-signed(d)) for d in distances]

    def far_line(expert):
        return far_code[pl.ds(expert, 1), :]

    def far_row_copy(i):
        d = NEAR[i]
        j = chunk_of(d)
        return remote(
            far_rows.at[pl.ds(CAP * i, CAP), :],
            r_buf.at[pl.ds(ROWS * j + PLACE[2], CAP), pl.ds(half, HALF)],
            fdsend_sem.at[i], fdrecv_sem.at[j],
            partner if d == 0 else at(dz=-signed(d), core=owner(d)),
        )

    def far_pick():
        for copy in far_copies():
            copy.wait_recv()
        pick = picks(far_line, far_experts(NEAR))
        for cols in (pl.ds(0, QUARTER), pl.ds(QUARTER, QUARTER)):
            far_rows[:, cols] = jnp.dot(pick, far_tok[:, cols], preferred_element_type=F32).astype(BF16)

        @pl.when(r == 0)
        def _():
            r_buf[pl.ds(PLACE[2], CAP), pl.ds(half, HALF)] = far_rows[pl.ds(0, CAP), :]

        @pl.when(r == 1)
        def _():
            far_row_copy(0).start()

        for i in (1, 2):
            far_row_copy(i).start()

    def far_pick_two():
        for i in range(3, len(NEAR)):
            far_row_copy(i).start()

    def z_arrived(k):
        pieces = z_pieces(k)
        if k == 3:
            pieces.sort(key=lambda piece: (piece[1], -piece[0]))
        for way, part in pieces:
            for copy in z_copies(k, way, part):
                copy.wait_recv()
            if k < ZN // 2 and (way, part) in z_pieces(k + 1):
                for copy in z_copies(k + 1, way, part):
                    copy.start()
            dispatch(k if way == 0 or k == ZN // 2 else ZN - k, (part,))

    def experts(*chunks):
        for core, j in enumerate(chunks):
            d = j if core == 0 else ZN - 1 - j

            @pl.when(r == core)
            def _():
                await_bytes(r_buf.at[pl.ds(ROWS * j, CAP), pl.ds(other, HALF)], yrecv0_sem.at[j])
                await_bytes(r_buf.at[pl.ds(ROWS * j + CAP, CAP * len(along_y(d))), :], yrecv_sem.at[j])
                if d == 0:
                    await_bytes(r_buf.at[pl.ds(ROWS * j + PLACE[2], CAP), pl.ds(other, HALF)], fdrecv_sem.at[j])
                elif d in NEAR:
                    await_bytes(r_buf.at[pl.ds(ROWS * j + PLACE[2], CAP), :], fdrecv_sem.at[j])

        rows = pl.ds(pl.multiple_of(ROWS * jnp.where(r == 0, chunks[0], chunks[1]), 16), ROWS)
        both = jnp.dot(r_buf[rows, :], wgu[...], preferred_element_type=F32)
        h_buf[...] = (jax.nn.silu(both[:, :FF]) * both[:, FF:]).astype(BF16)
        o_buf[rows, :] = jnp.dot(h_buf[...], wd[...], preferred_element_type=F32).astype(BF16)

    def back_copies(j, d):
        copies = []
        for k in back_along_y(d):
            for cols, core in ((half, r), (other, 1 - r)):
                copies.append(
                    remote(
                        o_buf.at[pl.ds(ROWS * j + PLACE[k], CAP), pl.ds(cols, HALF)],
                        q_buf.at[d, pl.ds(PLACE[k], CAP), :],
                        bsend_sem.at[j], brecv_sem.at[d], at(dy=-k, core=core),
                    )
                )
        return copies

    def back_own_copy(j, d):
        return remote(
            o_buf.at[pl.ds(ROWS * j, CAP), pl.ds(other, HALF)], q_buf.at[d, pl.ds(0, CAP), :],
            bsend0_sem.at[j], brecv0_sem.at[d], partner,
        )

    def far_back_copies(j, d):
        i = FAR.index(d)
        copies = []
        for cols, core in ((half, r), (other, 1 - r)):
            if d == 0 and core is r:
                continue
            copies.append(
                remote(
                    o_buf.at[pl.ds(ROWS * j + PLACE[2], CAP), pl.ds(cols, HALF)],
                    far_q.at[pl.ds(CAP * i, CAP), :],
                    fbsend_sem.at[j, 0 if core is r else 1], fbrecv_sem.at[i], at(dz=signed(d), core=core),
                )
            )
        return copies

    def give_back(*chunks):
        for core, j in enumerate(chunks):
            if j is None:
                continue
            d = j if core == 0 else ZN - 1 - j

            @pl.when(r == core)
            def _():
                for copy in back_copies(j, d):
                    copy.start()
                back_own_copy(j, d).start()
                q_buf[d, pl.ds(0, CAP), :] = o_buf[pl.ds(ROWS * j, CAP), pl.ds(half, HALF)]

    def give_far(*chunks):
        for core, j in enumerate(chunks):
            d = j if core == 0 else ZN - 1 - j

            @pl.when(r == core)
            def _():
                if d in FAR:
                    for copy in far_back_copies(j, d):
                        copy.start()
                if d == 0:
                    far_q[pl.ds(0, CAP), :] = o_buf[pl.ds(PLACE[2], CAP), pl.ds(half, HALF)]

    def far_out_copy():
        return remote(far_out, far_in, fsend_sem.at[2], frecv_sem.at[2], at(dy=2))

    def far_sum():
        @pl.when(r == 1)
        def _():
            await_bytes(far_q.at[pl.ds(0, CAP), :], fbrecv_sem.at[0])

        for i in range(1, len(FAR)):
            await_bytes(far_q.at[pl.ds(CAP * i, CAP), :], fbrecv_sem.at[i])
        spread = spreads(far_line, far_experts(FAR))
        for cols in (pl.ds(0, QUARTER), pl.ds(QUARTER, QUARTER)):
            far_out[:, cols] = lax.dot_general(
                spread, far_q[:, cols], (((0,), (0,)), ((), ())), preferred_element_type=F32
            ).astype(BF16)
        far_out_copy().start()

    def shared_copies():
        copies = []
        for k in range(1, XN):
            for crel, (cols, core) in enumerate(((half, r), (other, 1 - r))):
                copies.append(
                    remote(
                        sh_buf.at[pl.ds(TOK // 2 * k, TOK // 2), pl.ds(cols, HALF)],
                        s_in.at[k, pl.ds(here_rows, TOK // 2), :],
                        ssend_sem.at[k, crel], srecv_sem.at[0], at(dx=-k, core=core),
                    )
                )
        copies.append(
            remote(
                sh_buf.at[pl.ds(0, TOK // 2), pl.ds(other, HALF)],
                s_in.at[0, pl.ds(here_rows, TOK // 2), :],
                ssend_sem.at[0, 0], srecv_sem.at[1], partner,
            )
        )
        return copies

    def shared():
        for k in range(1, XN):
            x_copy(k).wait_recv()

        both = jnp.dot(t_buf[...], sgu[...], preferred_element_type=F32)
        sh_hidden[...] = (jax.nn.silu(both[:, : 2 * SF]) * both[:, 2 * SF :]).astype(BF16)
        sh_buf[...] = jnp.dot(sh_hidden[...], sd[...], preferred_element_type=F32).astype(BF16)
        for copy in shared_copies():
            copy.start()
        s_in[0, pl.ds(here_rows, TOK // 2), :] = sh_buf[pl.ds(0, TOK // 2), pl.ds(half, HALF)]

    def combined(d):
        await_bytes(q_buf.at[d, pl.ds(CAP, CAP * len(back_along_y(d))), :], brecv_sem.at[d])

        @pl.when(r != owner(d))
        def _():
            await_bytes(q_buf.at[d, pl.ds(0, CAP), :], brecv0_sem.at[d])

        spread = spreads(lambda expert: code[d, pl.ds(expert, 1), :], [expert_at(dy=k) for k in (0,) + back_along_y(d)])
        rows = pl.ds(0, CAP * (1 + len(back_along_y(d))))
        return [
            lax.dot_general(
                spread, q_buf[d, rows, pl.ds(part * QUARTER, QUARTER)], (((0,), (0,)), ((), ())),
                preferred_element_type=F32,
            )
            for part in range(2)
        ]

    def r_copy(step, way, part):
        outgoing, incoming = (plus_out, plus_in) if way == 0 else (minus_out, minus_in)
        cols = pl.ds(part * QUARTER, QUARTER)
        return remote(
            outgoing.at[step, :, cols], incoming.at[step, :, cols],
            rsend_sem.at[way, part, step], rrecv_sem.at[way, part, step], at(dz=1 if way == 0 else -1),
        )

    def loaded(first, last):
        for i in range(first, last):
            pltpu.make_async_copy(loads[i][0], loads[i][1], load_sem.at[i]).wait()
            weight_copy(i).wait_recv()

    dispatch(0)
    for copy in far_copies():
        copy.start()
    z_arrived(1)
    weight_copy(0).start()
    for k in range(1, XN):
        x_copy(k).start()
    z_arrived(2)
    weight_copy(1).start()
    weight_copy(2).start()
    z_arrived(3)
    loaded(0, 3)
    z_arrived(4)
    far_pick()
    far_pick_two()
    for i in range(3, 6):
        weight_copy(i).start()
    experts(0, 0)
    give_far(0, 0)
    experts(1, 2)
    give_far(1, 2)
    give_back(None, 2)
    experts(3, 3)
    give_far(3, 3)
    give_back(3, 3)
    experts(2, 1)
    give_far(2, 1)
    loaded(3, 6)
    shared()

    sums = combined(4)
    for way in range(2):
        outgoing = plus_out if way == 0 else minus_out
        outgoing[0, :, pl.ds(way * QUARTER, QUARTER)] = sums[way].astype(BF16)
        r_copy(0, way, way).start()
    give_back(2, 1)
    for step in range(1, 4):
        both = [combined(4 - step), combined(4 + step)]
        for i in range(2):
            for way in range(2):
                part = 1 - i if way == 0 else i
                outgoing, incoming = (plus_out, plus_in) if way == 0 else (minus_out, minus_in)
                cols = pl.ds(part * QUARTER, QUARTER)
                total = both[way][part]
                if step > 1 or part == way:
                    r_copy(step - 1, way, part).wait_recv()
                    total = total + incoming[step - 1, :, cols].astype(F32)
                outgoing[step, :, cols] = total.astype(BF16)
                r_copy(step, way, part).start()
            if step == 1 and i == 0:
                give_back(1, 0)
        if step == 1:
            give_back(0, None)
            far_sum()

    sums = combined(0)
    await_bytes(s_in.at[pl.ds(1, XN - 1)], srecv_sem.at[0])
    await_bytes(s_in.at[0, pl.ds(other_rows, TOK // 2), :], srecv_sem.at[1])
    far_out_copy().wait_recv()
    for part in range(2):
        cols = pl.ds(part * QUARTER, QUARTER)
        total = far_in[:, cols].astype(F32)
        for i in range(XN):
            total = total + s_in[i, :, cols].astype(F32)
        both[part] = total + sums[part]
    for way, part in ((0, 1), (1, 0), (0, 0), (1, 1)):
        r_copy(3, way, part).wait_recv()
        incoming = plus_in if way == 0 else minus_in
        both[part] = both[part] + incoming[3, :, pl.ds(part * QUARTER, QUARTER)].astype(F32)
    for part in range(2):
        out[:, pl.ds(part * QUARTER, QUARTER)] = both[part].astype(BF16)

    for i in range(6):
        weight_copy(i).wait_send()
    for k in range(1, XN):
        x_copy(k).wait_send()
    for k in range(1, ZN // 2 + 1):
        for piece in z_pieces(k):
            for copy in z_copies(k, *piece):
                copy.wait_send()
    for step in range(4):
        for piece in z_pieces(4 - step):
            r_copy(step, *piece).wait_send()
    for d in range(ZN):
        await_bytes(d_buf.at[d, pl.ds(CAP, CAP * len(along_y(d))), :], ysend_sem.at[d])

        @pl.when(r != owner(d))
        def _():
            await_bytes(d_buf.at[d, pl.ds(0, CAP), :], ysend0_sem.at[d])

    for j in range(ZN // 2):
        for core, d in ((0, j), (1, ZN - 1 - j)):

            @pl.when(r == core)
            def _():
                await_bytes(o_buf.at[pl.ds(ROWS * j + CAP, CAP * len(back_along_y(d))), :], bsend_sem.at[j])
                back_own_copy(j, d).wait_send()
                if d in FAR:
                    for copy in far_back_copies(j, d):
                        copy.wait_send()

    for copy in far_copies() + [far_out_copy()]:
        copy.wait_send()
    for i in range(1, len(NEAR)):
        far_row_copy(i).wait_send()

    @pl.when(r == 1)
    def _():
        far_row_copy(0).wait_send()

    for copy in shared_copies():
        copy.wait_send()


def on_device(*args):
    tokens, norm_gain, expert_ids, route_weights, *rest = args
    vmem = pl.BlockSpec(memory_space=pltpu.VMEM)
    hbm = pl.BlockSpec(memory_space=pl.ANY)
    dma = lambda *shape: pltpu.SemaphoreType.DMA(shape)
    half_z = ZN // 2
    return pl.pallas_call(
        kernel,
        out_shape=jax.ShapeDtypeStruct((TOK, HALF), BF16),
        in_specs=[vmem] * 4 + [hbm] * 6,
        out_specs=vmem,
        scratch_shapes=[
            pltpu.VMEM((XN * TOK // 2, D), BF16),
            pltpu.VMEM((ZN, TOK, HALF), BF16),
            pltpu.VMEM((ZN, EXPERTS, TOK), F32),
            pltpu.VMEM((ZN, ROWS, HALF), BF16),
            pltpu.VMEM((half_z * ROWS, D), BF16),
            pltpu.VMEM((ROWS, FF), BF16),
            pltpu.VMEM((half_z * ROWS, D), BF16),
            pltpu.VMEM((ZN, ROWS, HALF), BF16),
            pltpu.VMEM((TOK, HALF), BF16),
            pltpu.VMEM((EXPERTS, TOK), F32),
            pltpu.VMEM((CAP * len(NEAR), HALF), BF16),
            pltpu.VMEM((CAP * len(FAR), HALF), BF16),
            pltpu.VMEM((TOK, HALF), BF16),
            pltpu.VMEM((TOK, HALF), BF16),
            pltpu.VMEM((4, TOK, HALF), BF16),
            pltpu.VMEM((4, TOK, HALF), BF16),
            pltpu.VMEM((4, TOK, HALF), BF16),
            pltpu.VMEM((4, TOK, HALF), BF16),
            pltpu.VMEM((XN * TOK // 2, 2 * SF), BF16),
            pltpu.VMEM((XN * TOK // 2, D), BF16),
            pltpu.VMEM((XN, TOK, HALF), BF16),
            pltpu.VMEM((D, 2 * FF), BF16),
            pltpu.VMEM((FF, D), BF16),
            pltpu.VMEM((D, 4 * SF), BF16),
            pltpu.VMEM((2 * SF, D), BF16),
            dma(6), dma(6), dma(6),
            dma(2, 2, 4), dma(2, 2, 4), dma(2, 4), dma(2, 4),
            dma(ZN), dma(half_z), dma(ZN), dma(half_z),
            dma(half_z), dma(ZN), dma(half_z), dma(ZN),
            dma(2, 2, 4), dma(2, 2, 4),
            dma(3), dma(3), dma(XN, 2), dma(2),
            dma(3), dma(3), dma(len(NEAR)), dma(half_z), dma(half_z, 2), dma(len(FAR)),
        ],
        compiler_params=pltpu.CompilerParams(
            collective_id=0, has_side_effects=True, vmem_limit_bytes=63 * 2**20
        ),
    )(tokens, norm_gain, expert_ids.T, route_weights.T, *rest)


def solution(mesh):
    placed = (
        P(("dp", "expert"), None),
        P(),
        P(("dp", "expert"), None),
        P(("dp", "expert"), None),
        P("expert", None, "tensor"),
        P("expert", None, "tensor"),
        P("expert", "tensor", None),
        P(None, ("dp", "tensor")),
        P(None, ("dp", "tensor")),
        P(("dp", "tensor"), None),
    )
    return jax.shard_map(
        on_device,
        mesh=mesh,
        in_specs=placed,
        out_specs=P(("dp", "expert"), "tensor"),
        check_vma=False,
    )
```
